256 devices in a mesh: sx: 16 (over y, x), sy: 8 (over z), freq: 2 (over core).
Axes of the slice: x: 4, y: 4, z: 8, core: 2. Of those that a mesh axis runs over, the one named last changes fastest.
Arguments:
- update_basis: bfloat16 [4, 4096, 32, 1024], P('freq', ('sx', 'sy')), may hold values from -0.1875 to 0.1875
- update_coeff: bfloat16 [4, 4096, 32, 128], P('freq', ('sx', 'sy')), may hold values from -6 to 6
- owner: int32 [4096, 1], P(('sx', 'sy')), may hold values from 0 to 15; in each aligned block of 32 rows (0 to 31, 32 to 63, ...) at most 4 rows name the same one
- sep_rhs: bfloat16 [4, 16, 8, 1024, 128], P('freq', 'sx', 'sy'), may hold values from -6 to 6
- coupling: float32 [4, 16, 8, 4, 1024], P('freq', 'sx', 'sy'), may hold values from 0.1 to 0.25
- frontal_inverse: bfloat16 [4, 16, 8, 1024, 1024], P('freq', 'sx', 'sy'), may hold values from -0.2 to 1.2
Outputs:
- solution: float32 [4, 16, 8, 1024, 128], P('freq', 'sx', 'sy')
- residual_total: float32 [], replicated
The draws below stay inside these ranges and needn't reach their ends.
Inputs may be any that keep to these rules, and one draw needn't show every extreme that they name: In the 32 children of one grid position no owner appears more than 4 times; in every draw some owner appears exactly 4 times at some position.
All inputs are finite; a program needn't handle non-finite values.
Results may differ from the reference program's by a relative error of at most 0.0019.
Values may be sent and summed in bfloat16 or wider, within the bound.
No kernel may reach another device: no remote copies, remote signals or barrier semaphores. Data moves between devices by JAX's collectives and lax.ppermute only.
A program may use at most 128 MiB of HBM per device.

```python
import math
import jax
import jax.numpy as jnp
import numpy as np
from jax import lax

SEP = 1024
RANK = 32
NRHS = 128
C_DEV = 32
SWEEPS = 2
GRID_X = 16
GRID_Y = 8
CHILDREN = 4096
FREQS = 4
CAP = 4
N_SX = 16


def draw_frontal_inverse(key, part):
    first_key, second_key = jax.random.split(jax.random.fold_in(key, 7))
    spread = 0.35 * math.sqrt(3.0) / math.sqrt(SEP)
    matrix = jax.random.uniform(first_key, (FREQS, GRID_X, GRID_Y, SEP, SEP), jnp.float32, -spread, spread)
    diagonal = jax.random.uniform(second_key, (FREQS, GRID_X, GRID_Y, SEP), jnp.float32, 0.7, 0.9)
    positions = jnp.arange(SEP, dtype=jnp.int32)
    matrix = matrix.at[:, :, :, positions, positions].add(diagonal)
    return matrix.astype(jnp.bfloat16)


def block_scale(own_key, dims, pieces, low, top_value):
    factor_of = 1.0
    for dim, blocks in pieces:
        heights = jax.random.uniform(jax.random.fold_in(jax.random.fold_in(own_key, 6), dim), (blocks,), jnp.float32, low / len(pieces), top_value / len(pieces))
        factor_of = factor_of * jnp.repeat(jnp.exp(heights), dims[dim] // blocks).reshape((-1,) + (1,) * (len(dims) - 1 - dim))
    return factor_of


def shared_out(own_key, own, number, rows, amount, top, reach, lean):
    sequence = jax.random.permutation(own_key, amount)
    heavy_load, ordinary = load_shares(amount, rows * top, reach, lean, True), load_shares(amount, rows * top, reach, lean, False)
    places = jnp.arange(amount)

    def named(lengths, offset_by):
        used = int((lengths > 0).sum())
        fixed = max(1, used // 4)
        passed = fixed + (places - fixed + offset_by * (used - fixed)) % max(1, amount - fixed)
        return jnp.zeros((amount,), jnp.int32).at[sequence[jnp.where(places < fixed, places, passed)]].set(jnp.asarray(lengths, jnp.int32))

    lengths = jnp.where(number % 4 == 0, named(heavy_load, number // 4), named(ordinary, number - number // 4 - 1))
    mixed = jax.random.permutation(jax.random.fold_in(own, 3), amount)
    donor, receiver = mixed[0:amount // 2 * 2:2], mixed[1:amount // 2 * 2:2]
    margin = jnp.minimum(lengths[donor] - 1, reach - lengths[receiver]) // 2
    margin = jnp.where((donor == sequence[0]) | (receiver == sequence[0]) | (lengths[receiver] == 0), 0, jnp.maximum(margin, 0))
    passed = jax.random.randint(jax.random.fold_in(own, 4), (amount // 2,), 0, 1 << 20) % (margin + 1)
    lengths = lengths.at[donor].add(-passed).at[receiver].add(passed)
    members = jnp.searchsorted(jnp.cumsum(lengths), jnp.arange(rows * top), side="right").astype(jnp.int32)
    listing = members.reshape(top, rows).T
    listing = listing[jax.random.permutation(jax.random.fold_in(own, 1), rows)]
    offset_by = jax.random.randint(jax.random.fold_in(own, 2), (rows, 1), 0, top)
    return jnp.take_along_axis(listing, (jnp.arange(top)[None, :] + offset_by) % top, axis=1)


def load_shares(number_of, total, most, slope, full):
    weights = [(1 << 20) // math.isqrt(standing ** slope) + 1 for standing in range(1, number_of + 1)]
    largest = most if full else min(most, max(-(-total // number_of), total * weights[0] // sum(weights)))
    least = 1 if total - largest >= number_of - 1 else 0
    holding, rest = [largest] + [least] * (number_of - 1), total - largest - least * (number_of - 1)
    while rest > 0:
        free = [i for i in range(1, number_of) if holding[i] < largest] or [i for i in range(1, number_of) if holding[i] < most]
        pool, remaining = sum([weights[i] for i in free]), rest
        for i in free:
            more = min(most - holding[i], max(1, remaining * weights[i] // pool), rest)
            holding[i] = holding[i] + more
            rest = rest - more
    return np.array(holding)


def bell_draw(rng, dims, scale, bound, pieces=(), held_as=jnp.bfloat16):
    drawn = scale * jax.random.normal(rng, dims, jnp.float32)
    if pieces:
        drawn = drawn * block_scale(rng, dims, pieces, -0.22, 0.18)
    return jnp.clip(drawn, -bound, bound).astype(held_as)


def setup_inputs(seed: int = 0) -> dict:
    streams_of = jax.random.split(jax.random.key(seed), 7)
    update_basis = bell_draw(streams_of[0], (FREQS, CHILDREN, RANK, SEP), (RANK * C_DEV) ** -0.5, 0.1875, ((0, 2), (1, 128)))
    update_coeff = bell_draw(streams_of[1], (FREQS, CHILDREN, RANK, NRHS), 1.0, 6.0, ((0, 2), (1, 128)))
    owner_keys = jax.random.split(jax.random.fold_in(streams_of[2], 1), CHILDREN // C_DEV)
    owner_turns = jax.random.permutation(jax.random.fold_in(streams_of[2], 3), CHILDREN // C_DEV)
    owner = jax.vmap(lambda own, number: shared_out(jax.random.fold_in(streams_of[2], 2), own, number, C_DEV, N_SX, 1, CAP, 2))(owner_keys, owner_turns).reshape((CHILDREN, 1))
    sep_rhs = bell_draw(streams_of[3], (FREQS, GRID_X, GRID_Y, SEP, NRHS), 1.0, 6.0, ((0, 2), (1, 16), (2, 8)))
    coupling = jnp.clip(0.1 + 0.15 * jax.random.uniform(streams_of[4], (FREQS, GRID_X, GRID_Y, 4, SEP), jnp.float32) ** block_scale(streams_of[4], (FREQS, GRID_X, GRID_Y, 4, SEP), ((0, 2), (1, 16), (2, 8)), -0.2, 0.2), 0.1, 0.25)
    frontal_inverse = draw_frontal_inverse(jax.random.fold_in(streams_of[6], 71), 0)
    return dict(update_basis=update_basis, update_coeff=update_coeff, owner=owner, sep_rhs=sep_rhs, coupling=coupling, frontal_inverse=frontal_inverse)


def apply_inverse(frontal_inverse, field):
    rounded = lax.optimization_barrier(field.astype(jnp.bfloat16))

    def one_frequency(pair):
        matrix, vectors = pair
        return jnp.einsum('xyst,xytn->xysn', matrix.astype(jnp.float32), vectors.astype(jnp.float32))
    return lax.map(one_frequency, (frontal_inverse, rounded))

def neighbour_sum(field, coupling):
    padded = jnp.pad(field, ((0, 0), (1, 1), (1, 1), (0, 0), (0, 0)))
    result = coupling[:, :, :, 0, :, None] * padded[:, :-2, 1:-1]
    result = result + coupling[:, :, :, 1, :, None] * padded[:, 2:, 1:-1]
    result = result + coupling[:, :, :, 2, :, None] * padded[:, 1:-1, :-2]
    result = result + coupling[:, :, :, 3, :, None] * padded[:, 1:-1, 2:]
    return result

def reference(update_basis, update_coeff, owner, sep_rhs, coupling, frontal_inverse):
    blocks = CHILDREN // C_DEV
    owners = owner[:, 0].reshape(blocks, C_DEV)
    accumulated = jnp.zeros((FREQS, GRID_X, GRID_Y, SEP, NRHS), jnp.float32)

    def add_block(total, block_index):
        start = block_index * C_DEV
        basis_block = lax.dynamic_slice_in_dim(update_basis, start, C_DEV, 1).astype(jnp.float32)
        coeff_block = lax.dynamic_slice_in_dim(update_coeff, start, C_DEV, 1).astype(jnp.float32)
        products = jnp.einsum('fcrs,fcrn->fcsn', basis_block, coeff_block)
        targets = lax.dynamic_index_in_dim(owners, block_index, 0, keepdims=False)
        column = block_index % GRID_Y
        total = total.at[:, targets, column].add(products)
        return (total, None)
    accumulated, unused = lax.scan(add_block, accumulated, jnp.arange(blocks, dtype=jnp.int32))
    right_side = sep_rhs.astype(jnp.float32) - accumulated
    solution = apply_inverse(frontal_inverse, right_side)
    residual = right_side
    for sweep_index in range(SWEEPS):
        residual = right_side - solution + neighbour_sum(solution, coupling)
        solution = solution + apply_inverse(frontal_inverse, residual)
    weights = (jnp.arange(FREQS, dtype=jnp.float32) + 1.0) ** 2
    weighted_sum = jnp.sum(weights * lax.optimization_barrier(jnp.sum(residual * residual, axis=(1, 2, 3, 4))))
    residual_total = jnp.sqrt(weighted_sum / (FREQS * GRID_X * GRID_Y * SEP * NRHS) + 1e-06)
    return (solution, residual_total)
```

```python
import functools

import jax
import jax.numpy as jnp
from jax import lax
from jax.experimental import pallas as pl
from jax.experimental.pallas import tpu as pltpu
from jax.sharding import Mesh
from jax.sharding import PartitionSpec as P

SWEEPS = 2
SIDE = 4
CAP = 4
ROWS = 256
SX = ("sx_0", "sx_1")
SX_SY = ("sx_0", "sx_1", "sy")
ORDER = (0, 1, 3, 2)


def products_kernel(plan, owner_ref, place_ref, basis_ref, coeff_ref, *rest):
    outs = rest[: len(plan)]
    slots, used, stacked, weights = rest[len(plan) :]
    children = owner_ref.shape[0]
    rank = basis_ref.shape[2]
    rhs_count = coeff_ref.shape[3]
    step = pl.program_id(0)

    @pl.when(step == 0)
    def _():
        for o in range(SIDE * SIDE):
            used[o] = 0
        for s in range(SIDE * SIDE * CAP):
            slots[s] = children

        def put(c, carry):
            o = owner_ref[c]
            k = used[o]
            slots[o * CAP + k] = c
            used[o] = k + 1
            return carry

        lax.fori_loop(0, children, put, 0)
        weights[...] = jnp.zeros_like(weights)

    first = 0
    for out, (f, ahead, pairs) in zip(outs, plan, strict=True):
        for n, pair in enumerate(pairs):

            @pl.when(step == first + n)
            def _(out=out, f=f, ahead=ahead, pair=pair):
                for b, beside in enumerate(pair):
                    offsets = (ahead, beside) if f == 0 else (beside, ahead)
                    row = lax.rem(place_ref[0] + offsets[0], SIDE)
                    column = lax.rem(place_ref[1] + offsets[1], SIDE)
                    o = row * SIDE + column
                    for k in range(CAP):
                        c = slots[o * CAP + k]
                        filled = c < children
                        c = jnp.where(filled, c, 0)
                        at = (b * CAP + k) * rank
                        stacked[at : at + rank, :] = basis_ref[f, c]
                        coeff = coeff_ref[f, c]
                        weights[at : at + rank, b * rhs_count : (b + 1) * rhs_count] = jnp.where(
                            filled, coeff, jnp.zeros_like(coeff)
                        )
                for r in range(0, stacked.shape[1], ROWS):
                    product = lax.dot_general(
                        stacked[:, r : r + ROWS],
                        weights[...],
                        (((0,), (0,)), ((), ())),
                        preferred_element_type=jnp.float32,
                    )
                    for b in range(2):
                        piece = product[:, b * rhs_count : (b + 1) * rhs_count]
                        out[b, r : r + ROWS, :] = piece.astype(out.dtype)

        first += len(pairs)


def owner_products(plan, dtypes, owners, place, basis, coeff):
    f_local, children, rank, sep_size = basis.shape
    rhs_count = coeff.shape[3]
    steps = sum(len(pairs) for _, _, pairs in plan)
    out_specs, out_shape, first = [], [], 0
    for (_, _, pairs), dtype in zip(plan, dtypes, strict=True):
        out_specs.append(
            pl.BlockSpec(
                (2, sep_size, rhs_count),
                lambda i, *_, first=first, n=len(pairs): (jnp.clip(i - first, 0, n - 1), 0, 0),
            )
        )
        out_shape.append(jax.ShapeDtypeStruct((2 * len(pairs), sep_size, rhs_count), dtype))
        first += len(pairs)
    return pl.pallas_call(
        functools.partial(products_kernel, plan),
        grid_spec=pltpu.PrefetchScalarGridSpec(
            num_scalar_prefetch=2,
            grid=(steps,),
            in_specs=[
                pl.BlockSpec((f_local, children, rank, sep_size), lambda i, *_: (0, 0, 0, 0)),
                pl.BlockSpec((f_local, children, rank, rhs_count), lambda i, *_: (0, 0, 0, 0)),
            ],
            out_specs=out_specs,
            scratch_shapes=[
                pltpu.SMEM((SIDE * SIDE * CAP,), jnp.int32),
                pltpu.SMEM((SIDE * SIDE,), jnp.int32),
                pltpu.VMEM((2 * CAP * rank, sep_size), jnp.bfloat16),
                pltpu.VMEM((2 * CAP * rank, 2 * rhs_count), jnp.bfloat16),
            ],
        ),
        out_shape=out_shape,
        cost_estimate=pl.CostEstimate(
            flops=2 * steps * 4 * CAP * rank * sep_size * rhs_count * 2,
            bytes_accessed=basis.size * 2 + steps * 2 * sep_size * rhs_count * 2,
            transcendentals=0,
        ),
    )(owners, place, basis, coeff)


def turn(x, axis, by):
    return lax.ppermute(x, axis, [(i, (i + by) % SIDE) for i in range(SIDE)])


def add_into(x, index, y):
    return x.at[index].add(y)


def packed(x, power):
    scaled = (x * jnp.exp2(power)).astype(jnp.float16)
    tail = jnp.broadcast_to(power.astype(jnp.float16), (16, x.shape[1]))
    return jnp.concatenate([scaled, tail])


def unpacked(y):
    rows = y.shape[0] - 16
    power = y[rows, 0].astype(jnp.float32)
    return (y[:rows].astype(jnp.float32) * jnp.exp2(-power), power)


def summed(x, axis):
    copies = jnp.broadcast_to(x, (lax.axis_size(axis), *x.shape))
    return jnp.sum(lax.all_to_all(copies, axis, 0, 0, tiled=True), axis=0)


def neighbours(x, axis, count):
    up = [(i, i + 1) for i in range(count - 1)]
    return (lax.ppermute(x, axis, up), lax.ppermute(x, axis, [(b, a) for a, b in up]))


def on_device(update_basis, update_coeff, owner, sep_rhs, coupling, frontal_inverse):
    f_local = update_basis.shape[0]
    sep_size = update_basis.shape[3]
    rhs_count = update_coeff.shape[3]
    columns = lax.axis_size(SX)
    place = jnp.stack([lax.axis_index("sx_0"), lax.axis_index("sx_1")]).astype(jnp.int32)
    owners = owner[:, 0]

    plan = tuple((f, 2, (pair,)) for f in range(2) for pair in ((0, 1), (3, 2)))
    far = owner_products(plan, (jnp.bfloat16,) * 4, owners, place, update_basis, update_coeff)
    plan = tuple((f, ahead, ((0, 1), (3, 2))) for f in range(2) for ahead in (1, 3, 0))
    dtypes = (jnp.bfloat16, jnp.bfloat16, jnp.float32) * 2
    near = owner_products(plan, dtypes, owners, place, update_basis, update_coeff)

    axes = (("sx_0", "sx_1"), ("sx_1", "sx_0"))
    half = sep_size // 2
    contribution = []
    got = [(turn(far[2 * f], axes[f][0], 1), turn(far[2 * f + 1], axes[f][0], -1)) for f in range(2)]
    sums = []
    for f in range(2):
        following, preceding, own = near[3 * f : 3 * f + 3]
        following = add_into(following, slice(0, 2), got[f][0])
        preceding = add_into(preceding, slice(2, 4), got[f][1])
        a = turn(following, axes[f][0], 1)
        b = turn(preceding, axes[f][0], -1)
        sums.append((a, b, own))
    for f in range(2):
        a, b, own = sums[f]
        total = [own[i] + a[i].astype(jnp.float32) + b[i].astype(jnp.float32) for i in range(4)]
        axis = axes[f][1]
        largest = functools.reduce(jnp.maximum, [jnp.max(jnp.abs(part)) for part in total[1:]])
        power = jnp.clip(14.0 - jnp.ceil(jnp.log2(largest)), -60.0, 100.0)
        a, a_power = unpacked(turn(packed(total[3][:half], power), axis, 1))
        b, b_power = unpacked(turn(packed(total[3][half:], power), axis, -1))
        following = jnp.concatenate([total[1][:half] + a, total[1][half:]])
        preceding = jnp.concatenate([total[2][:half], total[2][half:] + b])
        a, _ = unpacked(turn(packed(following, jnp.minimum(power, a_power)), axis, 1))
        b, _ = unpacked(turn(packed(preceding, jnp.minimum(power, b_power)), axis, -1))
        contribution.append(total[0] + a + b)
    contribution = jnp.stack(contribution)

    right_side = sep_rhs[:, 0, 0].astype(jnp.float32) - contribution
    inverse_block = frontal_inverse[:, 0, 0]
    coupling_rows = coupling[:, 0, 0]

    def apply_inverse(field):
        return jnp.einsum(
            "fst,ftn->fsn",
            inverse_block,
            field.astype(jnp.bfloat16),
            preferred_element_type=jnp.float32,
        )

    solution = apply_inverse(right_side)
    residual = right_side
    for _ in range(SWEEPS):
        sent = solution.astype(jnp.bfloat16)
        around = neighbours(sent, SX, columns) + neighbours(sent, "sy", lax.axis_size("sy"))
        residual = right_side - solution
        for d in range(4):
            residual = residual + coupling_rows[:, d, :, None] * around[d].astype(jnp.float32)
        solution = solution + apply_inverse(residual)
    freq_ids = lax.axis_index("freq") * f_local + jnp.arange(f_local, dtype=jnp.int32) + 1
    weights = freq_ids.astype(jnp.float32) ** 2
    weighted_sum = jnp.sum(weights * jnp.sum(residual * residual, axis=(1, 2)))
    spread = jnp.broadcast_to(weighted_sum, (8, rhs_count))
    spread = spread + lax.ppermute(spread, "freq", [(0, 1), (1, 0)])
    spread = summed(spread, "sy")
    weighted_sum = summed(spread, SX)[0, 0]
    entries = float(
        f_local * lax.axis_size("freq") * columns * lax.axis_size("sy") * sep_size * rhs_count
    )
    residual_total = jnp.sqrt(weighted_sum / entries + 1e-06)
    return (solution[:, None, None], residual_total)


def solution(mesh):
    finer = Mesh(
        mesh.devices.reshape(SIDE, SIDE, mesh.shape["sy"], mesh.shape["freq"]),
        ("sx_0", "sx_1", "sy", "freq"),
    )
    return jax.shard_map(
        on_device,
        mesh=finer,
        in_specs=(
            P("freq", SX_SY, None, None),
            P("freq", SX_SY, None, None),
            P(SX_SY, None),
            P("freq", SX, "sy", None, None),
            P("freq", SX, "sy", None, None),
            P("freq", SX, "sy", None, None),
        ),
        out_specs=(P("freq", SX, "sy", None, None), P()),
        check_vma=False,
    )
```

```python
import functools

import jax
import jax.numpy as jnp
from jax import lax
from jax.experimental import pallas as pl
from jax.experimental.pallas import tpu as pltpu
from jax.sharding import Mesh
from jax.sharding import PartitionSpec as P


SWEEPS = 2
SIDE = 4
CAP = 4
TILE = 256
SX = ("sx_0", "sx_1")
SX_SY = ("sx_0", "sx_1", "sy")
LOW, HIGH = (0, 1), (3, 2)


def cost(flops, bytes_accessed):
    return pl.CostEstimate(flops=flops, bytes_accessed=bytes_accessed, transcendentals=0)


def room(mebibytes):
    return pltpu.CompilerParams(vmem_limit_bytes=mebibytes << 20)


def products_kernel(plan, owner_ref, place_ref, basis_ref, coeff_ref, *rest):
    outs = rest[: len(plan)]
    slots, used, stacked, weights = rest[-4:]
    children = owner_ref.shape[0]
    rank = basis_ref.shape[2]
    rhs_count = coeff_ref.shape[3]
    step = pl.program_id(0)

    @pl.when(step == 0)
    def _():
        for o in range(SIDE * SIDE):
            used[o] = 0
        for s in range(SIDE * SIDE * CAP):
            slots[s] = children

        def put(c, carry):
            o = owner_ref[c]
            k = used[o]
            slots[o * CAP + k] = c
            used[o] = k + 1
            return carry

        lax.fori_loop(0, children, put, 0)
        weights[...] = jnp.zeros_like(weights)

    first = 0
    for out, (f, ahead, pairs) in zip(outs, plan, strict=True):
        for n, pair in enumerate(pairs):

            @pl.when(step == first + n)
            def _(out=out, f=f, ahead=ahead, pair=pair):
                for b, beside in enumerate(pair):
                    offsets = (ahead, beside) if f == 0 else (beside, ahead)
                    row = lax.rem(place_ref[0] + offsets[0], SIDE)
                    column = lax.rem(place_ref[1] + offsets[1], SIDE)
                    o = row * SIDE + column
                    for k in range(CAP):
                        c = slots[o * CAP + k]
                        filled = c < children
                        c = jnp.where(filled, c, 0)
                        at = (b * CAP + k) * rank
                        stacked[at : at + rank, :] = basis_ref[f, c]
                        coeff = coeff_ref[f, c]
                        weights[at : at + rank, b * rhs_count : (b + 1) * rhs_count] = jnp.where(
                            filled, coeff, jnp.zeros_like(coeff)
                        )
                turned = weights[...].T
                for s in range(0, stacked.shape[1], TILE):
                    product = jnp.dot(
                        turned, stacked[:, s : s + TILE], preferred_element_type=jnp.float32
                    )
                    for b in range(2):
                        piece = product[b * rhs_count : (b + 1) * rhs_count]
                        out[b, :, s : s + TILE] = piece.astype(out.dtype)

        first += len(pairs)


def owner_products(plan, dtypes, owners, place, basis, coeff, after=(), skipped=None):
    f_local, children, rank, sep_size = basis.shape
    rhs_count = coeff.shape[3]
    steps = sum(len(pairs) for _, _, pairs in plan)
    out_specs, out_shape, first, written = [], [], 0, 0
    for at, ((_, _, pairs), dtype) in enumerate(zip(plan, dtypes, strict=True)):
        n, base = len(pairs), skipped[at] if skipped else 0
        out_specs.append(
            pl.BlockSpec(
                (2, rhs_count, sep_size),
                lambda i, *_, first=first, n=n, base=base: (jnp.clip(i - first, 0, n - 1) + base, 0, 0),
            )
        )
        out_shape.append(jax.ShapeDtypeStruct((2 * (n + base), rhs_count, sep_size), dtype))
        written += 2 * n * rhs_count * sep_size * jnp.dtype(dtype).itemsize
        first += n

    def body(owner_ref, place_ref, basis_ref, coeff_ref, *rest):
        products_kernel(plan, owner_ref, place_ref, basis_ref, coeff_ref, *rest[len(after) :])

    return pl.pallas_call(
        body,
        grid_spec=pltpu.PrefetchScalarGridSpec(
            num_scalar_prefetch=2,
            grid=(steps,),
            in_specs=[
                pl.BlockSpec((f_local, children, rank, sep_size), lambda i, *_: (0, 0, 0, 0)),
                pl.BlockSpec((f_local, children, rank, rhs_count), lambda i, *_: (0, 0, 0, 0)),
            ]
            + [pl.BlockSpec(memory_space=pl.ANY) for _ in after],
            out_specs=out_specs,
            scratch_shapes=[
                pltpu.SMEM((SIDE * SIDE * CAP,), jnp.int32),
                pltpu.SMEM((SIDE * SIDE,), jnp.int32),
                pltpu.VMEM((2 * CAP * rank, sep_size), jnp.bfloat16),
                pltpu.VMEM((2 * CAP * rank, 2 * rhs_count), jnp.bfloat16),
            ],
        ),
        out_shape=out_shape,
        compiler_params=room(32),
        cost_estimate=cost(
            2 * steps * 4 * CAP * rank * sep_size * rhs_count * 2, basis.size * 2 + written
        ),
    )(owners, place, basis, coeff, *after)


def join(mine, got, whole):
    def body(mine_ref, got_ref, whole_ref, out_ref):
        out_ref[...] = (mine_ref[...] + got_ref[...].astype(jnp.float32)).astype(out_ref.dtype)

    n = mine.shape[0]
    block = (1, *mine.shape[1:])
    spec = pl.BlockSpec(block, lambda i: (i, 0, 0))
    return pl.pallas_call(
        body,
        grid=(n,),
        in_specs=[spec, spec, pl.BlockSpec(memory_space=pl.ANY)],
        out_specs=spec,
        out_shape=jax.ShapeDtypeStruct(whole.shape, whole.dtype),
        input_output_aliases={2: 0},
        compiler_params=room(8),
        cost_estimate=cost(mine.size * 2, mine.size * 8),
    )(mine, got, whole)


def row_totals(own, low, high):
    _, rhs_count, sep_size = own.shape
    half = rhs_count // 2

    def body(own_ref, low_ref, high_ref, here, following, preceding, one_way, other_way):
        def total(at):
            crossed = (at + 2) % SIDE
            return own_ref[at] + low_ref[at].astype(jnp.float32) + high_ref[crossed].astype(jnp.float32)

        here[...] = total(0)
        following[...] = total(1)
        preceding[...] = total(2)
        opposite = total(3).astype(jnp.bfloat16)
        one_way[...] = opposite[:half]
        other_way[...] = opposite[half:]

    whole = jax.ShapeDtypeStruct((rhs_count, sep_size), jnp.float32)
    part = jax.ShapeDtypeStruct((half, sep_size), jnp.bfloat16)
    stack = pl.BlockSpec((SIDE, rhs_count, TILE), lambda i: (0, 0, i))
    return pl.pallas_call(
        body,
        grid=(sep_size // TILE,),
        in_specs=[stack] * 3,
        out_specs=[pl.BlockSpec((rhs_count, TILE), lambda i: (0, i))] * 3
        + [pl.BlockSpec((half, TILE), lambda i: (0, i))] * 2,
        out_shape=[whole] * 3 + [part] * 2,
        compiler_params=room(12),
        cost_estimate=cost(own.size * 2, own.size * 12),
    )(own, low, high)


def join_half(whole, got, which):
    half = whole.shape[0] // 2

    def body(mine_ref, got_ref, out_ref):
        out_ref[...] = mine_ref[...] + got_ref[...].astype(jnp.float32)

    return pl.pallas_call(
        body,
        grid=(2,),
        in_specs=[
            pl.BlockSpec((half // 2, whole.shape[1]), lambda i: (2 * which + i, 0)),
            pl.BlockSpec((half // 2, whole.shape[1]), lambda i: (i, 0)),
        ],
        out_specs=pl.BlockSpec((half // 2, whole.shape[1]), lambda i: (2 * which + i, 0)),
        out_shape=jax.ShapeDtypeStruct(whole.shape, whole.dtype),
        input_output_aliases={0: 0},
        compiler_params=room(6),
        cost_estimate=cost(got.size, got.size * 10),
    )(whole, got)


def across(field, matrix_tile):
    return lax.dot_general(
        field, matrix_tile, (((1,), (1,)), ((), ())), preferred_element_type=jnp.float32
    )


def field_spec(rhs_count, sep_size):
    return pl.BlockSpec((1, rhs_count, sep_size), lambda f, i: (f, 0, 0))


def tile_spec(rhs_count):
    return pl.BlockSpec((1, rhs_count, TILE), lambda f, i: (f, 0, i))


def matrix_spec(sep_size):
    return pl.BlockSpec((1, TILE, sep_size), lambda f, i: (f, i, 0))


def first_solve(sep_rhs, parts, matrix):
    f_local, sep_size, _ = matrix.shape
    rhs_count = sep_rhs.shape[2]

    def body(rhs_ref, *rest):
        parts_refs, (matrix_ref, right_ref, out_ref, sent_ref, field) = rest[:6], rest[6:]
        f, i = pl.program_id(0), pl.program_id(1)
        for g in range(2):

            @pl.when((i == 0) & (f == g))
            def _(g=g):
                here, low, high = parts_refs[3 * g : 3 * g + 3]
                right = rhs_ref[0].astype(jnp.float32).T - (here[...] + low[...] + high[...])
                right_ref[0] = right
                field[...] = right.astype(jnp.bfloat16)

        out = across(field[...], matrix_ref[0])
        out_ref[0] = out
        sent_ref[0] = out.astype(jnp.bfloat16)

    whole = pl.BlockSpec((rhs_count, sep_size), lambda f, i: (0, 0))
    shape = (f_local, rhs_count, sep_size)
    return pl.pallas_call(
        body,
        grid=(f_local, sep_size // TILE),
        in_specs=[pl.BlockSpec((1, sep_size, rhs_count), lambda f, i: (f, 0, 0))]
        + [whole] * 6
        + [matrix_spec(sep_size)],
        out_specs=[field_spec(rhs_count, sep_size), tile_spec(rhs_count), tile_spec(rhs_count)],
        out_shape=[
            jax.ShapeDtypeStruct(shape, jnp.float32),
            jax.ShapeDtypeStruct(shape, jnp.float32),
            jax.ShapeDtypeStruct(shape, jnp.bfloat16),
        ],
        scratch_shapes=[pltpu.VMEM((rhs_count, sep_size), jnp.bfloat16)],
        compiler_params=room(16),
        cost_estimate=cost(2 * matrix.size * rhs_count, matrix.size * 2 + sep_rhs.size * 24),
    )(sep_rhs, *parts, matrix)


def residual_of(right_ref, mine_ref, coupling_ref, around):
    residual = right_ref[0] - mine_ref[0]
    for d in range(4):
        residual = residual + coupling_ref[0, d : d + 1, :] * around[d][0].astype(jnp.float32)
    return residual


def sweep(right_side, mine, around, coupling, matrix):
    f_local, sep_size, _ = matrix.shape
    rhs_count = mine.shape[1]

    def body(right_ref, whole_ref, *rest):
        around_refs, (coupling_ref, matrix_ref, mine_ref, out_ref, sent_ref, field) = rest[:4], rest[4:]

        @pl.when(pl.program_id(1) == 0)
        def _():
            field[...] = residual_of(right_ref, whole_ref, coupling_ref, around_refs).astype(jnp.bfloat16)

        out = mine_ref[0] + across(field[...], matrix_ref[0])
        out_ref[0] = out
        sent_ref[0] = out.astype(jnp.bfloat16)

    return pl.pallas_call(
        body,
        grid=(f_local, sep_size // TILE),
        in_specs=[field_spec(rhs_count, sep_size)] * 6
        + [pl.BlockSpec((1, 4, sep_size), lambda f, i: (f, 0, 0)), matrix_spec(sep_size), tile_spec(rhs_count)],
        out_specs=[tile_spec(rhs_count)] * 2,
        out_shape=[
            jax.ShapeDtypeStruct(mine.shape, jnp.float32),
            jax.ShapeDtypeStruct(mine.shape, jnp.bfloat16),
        ],
        scratch_shapes=[pltpu.VMEM((rhs_count, sep_size), jnp.bfloat16)],
        compiler_params=room(12),
        cost_estimate=cost(2 * matrix.size * rhs_count, matrix.size * 2 + mine.size * 24),
    )(right_side, mine, *around, coupling, matrix, mine)


def last_residual(weights, right_side, mine, around, coupling, copies):
    f_local, rhs_count, sep_size = mine.shape

    def body(weight_ref, right_ref, mine_ref, *rest):
        around_refs, (coupling_ref, field_ref, sum_ref, total) = rest[:4], rest[4:]
        f = pl.program_id(0)
        residual = residual_of(right_ref, mine_ref, coupling_ref, around_refs)
        field_ref[0] = residual.astype(jnp.bfloat16)
        square = jnp.sum(residual * residual, axis=0, keepdims=True) * weight_ref[f]

        @pl.when(f == 0)
        def _():
            total[...] = square

        @pl.when(f > 0)
        def _():
            total[...] += square

        @pl.when(f == f_local - 1)
        def _():
            sum_ref[...] = jnp.broadcast_to(jnp.sum(total[...]), sum_ref.shape)

    spec = pl.BlockSpec((1, rhs_count, sep_size), lambda f, *_: (f, 0, 0))
    return pl.pallas_call(
        body,
        grid_spec=pltpu.PrefetchScalarGridSpec(
            num_scalar_prefetch=1,
            grid=(f_local,),
            in_specs=[spec] * 6 + [pl.BlockSpec((1, 4, sep_size), lambda f, *_: (f, 0, 0))],
            out_specs=[spec, pl.BlockSpec((copies, 8, 128), lambda f, *_: (0, 0, 0))],
            scratch_shapes=[pltpu.VMEM((1, sep_size), jnp.float32)],
        ),
        out_shape=[
            jax.ShapeDtypeStruct(mine.shape, jnp.bfloat16),
            jax.ShapeDtypeStruct((copies, 8, 128), jnp.float32),
        ],
        compiler_params=room(12),
        cost_estimate=cost(mine.size * 12, mine.size * 18),
    )(weights, right_side, mine, *around, coupling)


def last_solve(mine, field, matrix):
    f_local, sep_size, _ = matrix.shape
    rhs_count = mine.shape[1]

    def body(mine_ref, field_ref, matrix_ref, out_ref):
        out_ref[0] = mine_ref[0].T + across(matrix_ref[0], field_ref[0])

    return pl.pallas_call(
        body,
        grid=(f_local, sep_size // TILE),
        in_specs=[tile_spec(rhs_count), field_spec(rhs_count, sep_size), matrix_spec(sep_size)],
        out_specs=pl.BlockSpec((1, TILE, rhs_count), lambda f, i: (f, i, 0)),
        out_shape=jax.ShapeDtypeStruct((f_local, sep_size, rhs_count), jnp.float32),
        compiler_params=room(10),
        cost_estimate=cost(2 * matrix.size * rhs_count, matrix.size * 2 + mine.size * 10),
    )(mine, field, matrix)


def turn(x, axis, by):
    return lax.ppermute(x, axis, [(i, (i + by) % SIDE) for i in range(SIDE)])


def neighbours(x, axis, count):
    up = [(i, i + 1) for i in range(count - 1)]
    return (lax.ppermute(x, axis, up), lax.ppermute(x, axis, [(b, a) for a, b in up]))


def on_device(update_basis, update_coeff, owner, sep_rhs, coupling, frontal_inverse):
    f_local = update_basis.shape[0]
    sep_size = update_basis.shape[3]
    rhs_count = update_coeff.shape[3]
    columns, rows = lax.axis_size(SX), lax.axis_size("sy")
    place = jnp.stack([lax.axis_index("sx_0"), lax.axis_index("sx_1")]).astype(jnp.int32)
    owners = owner[:, 0]
    data = (owners, place, update_basis, update_coeff)

    axes = (SX, SX[::-1])
    plan = tuple((f, 2, (pair,)) for f in range(2) for pair in (LOW, HIGH))
    far = owner_products(plan, (jnp.bfloat16,) * 4, *data)
    got = [(turn(far[2 * f], axes[f][0], 1), turn(far[2 * f + 1], axes[f][0], -1)) for f in range(2)]

    plan = tuple(
        (f, ahead, (pair,)) for f in range(2) for ahead, pair in ((1, LOW), (3, HIGH))
    ) + tuple((f, ahead, (pair,)) for f in range(2) for ahead, pair in ((1, HIGH), (3, LOW)))
    dtypes = (jnp.float32,) * 4 + (jnp.bfloat16,) * 4
    near = owner_products(plan, dtypes, *data, skipped=(0,) * 4 + (1,) * 4)

    sums, joined = [], []
    for f in range(2):
        following = join(near[2 * f], got[f][0], near[4 + 2 * f])
        preceding = join(near[2 * f + 1], got[f][1], near[5 + 2 * f])
        joined += [following, preceding]
        sums.append((turn(following, axes[f][0], 1), turn(preceding, axes[f][0], -1)))
    plan = tuple((f, 0, (LOW, HIGH)) for f in range(2))
    own = owner_products(plan, (jnp.float32,) * 2, *data, after=tuple(joined))

    parts = []
    for f in range(2):
        here, following, preceding, one_way, other_way = row_totals(own[f], *sums[f])
        axis = axes[f][1]
        a, b = turn(one_way, axis, 1), turn(other_way, axis, -1)
        following = join_half(following, a, 0)
        preceding = join_half(preceding, b, 1)
        parts += [here, turn(following, axis, 1), turn(preceding, axis, -1)]

    matrix = frontal_inverse[:, 0, 0]
    coupling_rows = coupling[:, 0, 0]
    right_side, mine, sent = first_solve(sep_rhs[:, 0, 0], parts, matrix)
    for _ in range(SWEEPS - 1):
        around = neighbours(sent, SX, columns) + neighbours(sent, "sy", rows)
        mine, sent = sweep(right_side, mine, around, coupling_rows, matrix)
    around = neighbours(sent, SX, columns) + neighbours(sent, "sy", rows)
    freq_ids = lax.axis_index("freq") * f_local + jnp.arange(f_local, dtype=jnp.int32) + 1
    weights = freq_ids.astype(jnp.float32) ** 2
    group = ("sy", "freq")
    field, squares = last_residual(
        weights, right_side, mine, around, coupling_rows, lax.axis_size(group)
    )
    squares = jnp.sum(lax.all_to_all(squares, group, 0, 0, tiled=True), axis=0)
    squares = jnp.broadcast_to(squares, (columns, *squares.shape))
    squares = jnp.sum(lax.all_to_all(squares, SX, 0, 0, tiled=True), axis=0)
    weighted_sum = squares[0, 0]
    solution = last_solve(mine, field, matrix)
    entries = float(f_local * lax.axis_size("freq") * columns * rows * sep_size * rhs_count)
    residual_total = jnp.sqrt(weighted_sum / entries + 1e-06)
    return (solution[:, None, None], residual_total)


def solution(mesh):
    finer = Mesh(
        mesh.devices.reshape(SIDE, SIDE, mesh.shape["sy"], mesh.shape["freq"]),
        ("sx_0", "sx_1", "sy", "freq"),
    )
    return jax.shard_map(
        on_device,
        mesh=finer,
        in_specs=(
            P("freq", SX_SY, None, None),
            P("freq", SX_SY, None, None),
            P(SX_SY, None),
            P("freq", SX, "sy", None, None),
            P("freq", SX, "sy", None, None),
            P("freq", SX, "sy", None, None),
        ),
        out_specs=(P("freq", SX, "sy", None, None), P()),
        check_vma=False,
    )
```

```python
import functools

import jax
import jax.numpy as jnp
from jax import lax
from jax.experimental import pallas as pl
from jax.experimental.pallas import tpu as pltpu
from jax.sharding import Mesh
from jax.sharding import PartitionSpec as P


SWEEPS = 2
SIDE = 4
CAP = 4
TILE = 256
SX = ("sx_0", "sx_1")
SX_SY = ("sx_0", "sx_1", "sy")
LOW, HIGH = (0, 1), (3, 2)


def cost(flops, bytes_accessed):
    return pl.CostEstimate(flops=flops, bytes_accessed=bytes_accessed, transcendentals=0)


def room(mebibytes):
    return pltpu.CompilerParams(vmem_limit_bytes=mebibytes << 20)


def fill_slots(owner_ref, slots, used):
    children = owner_ref.shape[0]
    for o in range(SIDE * SIDE):
        used[o] = 0
    for s in range(SIDE * SIDE * CAP):
        slots[s] = children

    def put(c, carry):
        o = owner_ref[c]
        k = used[o]
        slots[o * CAP + k] = c
        used[o] = k + 1
        return carry

    lax.fori_loop(0, children, put, 0)


def owner_at(table_ref, f, ahead, beside):
    offsets = (ahead, beside) if f == 0 else (beside, ahead)
    row = lax.rem(table_ref[0] + offsets[0], SIDE)
    column = lax.rem(table_ref[1] + offsets[1], SIDE)
    return row * SIDE + column


def multiply(weights, stacked, out, at):
    rhs_count = out.shape[1]
    turned = weights[...].T
    for s in range(0, stacked.shape[1], TILE):
        product = jnp.dot(turned, stacked[:, s : s + TILE], preferred_element_type=jnp.float32)
        for b in range(2):
            piece = product[b * rhs_count : (b + 1) * rhs_count]
            out[at + b, :, s : s + TILE] = piece.astype(out.dtype)


def put_weights(weights, coeff_ref, f, c, filled, b, k):
    rank, rhs_count = coeff_ref.shape[2:]
    at = (b * CAP + k) * rank
    coeff = coeff_ref[f, c]
    weights[at : at + rank, b * rhs_count : (b + 1) * rhs_count] = jnp.where(
        filled, coeff, jnp.zeros_like(coeff)
    )


def owner_products(plan, shapes, owners, place, basis, coeff, after=(), fetched=False):
    _, children, rank, sep_size = basis.shape
    rhs_count = coeff.shape[3]
    count = len(plan) if fetched else 1
    depth = 2 * CAP * rank

    def body(owner_ref, table_ref, basis_ref, coeff_ref, *rest):
        outs = rest[len(after) : len(after) + len(shapes)]
        slots, used, stacked, weights = rest[len(after) + len(shapes) :][:4]
        arrived = rest[-1]
        fill_slots(owner_ref, slots, used)

        def child(f, ahead, beside, k):
            c = slots[owner_at(table_ref, f, ahead, beside) * CAP + k]
            filled = c < children
            return jnp.where(filled, c, 0), filled

        def copies(n):
            _, _, f, ahead, pair = plan[n]
            return [
                pltpu.make_async_copy(
                    basis_ref.at[f, child(f, ahead, beside, k)[0]],
                    stacked.at[n, pl.ds((b * CAP + k) * rank, rank)],
                    arrived.at[n],
                )
                for b, beside in enumerate(pair)
                for k in range(CAP)
            ]

        if fetched:
            flights = [copies(n) for n in range(len(plan))]
            for flight in flights:
                for copy in flight:
                    copy.start()
        weights[...] = jnp.zeros_like(weights)
        for n, (out, at, f, ahead, pair) in enumerate(plan):
            for b, beside in enumerate(pair):
                for k in range(CAP):
                    c, filled = child(f, ahead, beside, k)
                    put_weights(weights, coeff_ref, f, c, filled, b, k)
                    if not fetched:
                        stacked[0, pl.ds((b * CAP + k) * rank, rank)] = basis_ref[f, c]
            if fetched:
                for copy in flights[n]:
                    copy.wait()
            multiply(weights, stacked.at[n if fetched else 0], outs[out], at)

    space = pltpu.MemorySpace.HBM if fetched else pltpu.MemorySpace.VMEM
    return pl.pallas_call(
        body,
        in_specs=[pl.BlockSpec(memory_space=pltpu.MemorySpace.SMEM)] * 2
        + [pl.BlockSpec(memory_space=space), pl.BlockSpec(memory_space=pltpu.MemorySpace.VMEM)]
        + [pl.BlockSpec(memory_space=pl.ANY) for _ in after],
        out_specs=[pl.BlockSpec(memory_space=pltpu.MemorySpace.VMEM) for _ in shapes],
        scratch_shapes=[
            pltpu.SMEM((SIDE * SIDE * CAP,), jnp.int32),
            pltpu.SMEM((SIDE * SIDE,), jnp.int32),
            pltpu.VMEM((count, depth, sep_size), jnp.bfloat16),
            pltpu.VMEM((depth, 2 * rhs_count), jnp.bfloat16),
            pltpu.SemaphoreType.DMA((count,)),
        ],
        out_shape=[jax.ShapeDtypeStruct((n, rhs_count, sep_size), dtype) for n, dtype in shapes],
        compiler_params=room(57 if fetched else 16),
        cost_estimate=cost(
            2 * len(plan) * 4 * CAP * rank * sep_size * rhs_count * 2,
            len(plan) * 2 * (CAP * rank * sep_size * 2 + rhs_count * sep_size * 4),
        ),
    )(owners, place, basis, coeff, *after)


def in_vmem(count):
    return [pl.BlockSpec(memory_space=pltpu.MemorySpace.VMEM)] * count


def join(mine, got, whole):
    def body(mine_ref, got_ref, whole_ref, out_ref):
        n = mine_ref.shape[0]
        out_ref[:n] = (mine_ref[...] + got_ref[...].astype(jnp.float32)).astype(out_ref.dtype)

    return pl.pallas_call(
        body,
        in_specs=in_vmem(3),
        out_specs=in_vmem(1)[0],
        out_shape=jax.ShapeDtypeStruct(whole.shape, whole.dtype),
        input_output_aliases={2: 0},
        compiler_params=room(4),
        cost_estimate=cost(mine.size * 2, mine.size * 8),
    )(mine, got, whole)


def row_totals(own, low, high):
    _, rhs_count, sep_size = own.shape

    def body(own_ref, low_ref, high_ref, *outs):
        for at, out in enumerate(outs):
            crossed = (at + 2) % SIDE
            total = own_ref[at] + low_ref[at].astype(jnp.float32) + high_ref[crossed].astype(jnp.float32)
            out[...] = total.astype(out.dtype)

    types = (jnp.float32,) * 3 + (jnp.bfloat16,)
    return pl.pallas_call(
        body,
        in_specs=in_vmem(3),
        out_specs=in_vmem(SIDE),
        out_shape=[jax.ShapeDtypeStruct((rhs_count, sep_size), dtype) for dtype in types],
        compiler_params=room(4),
        cost_estimate=cost(own.size * 2, own.size * 12),
    )(own, low, high)


def across(field, matrix_tile):
    return lax.dot_general(
        field, matrix_tile, (((1,), (1,)), ((), ())), preferred_element_type=jnp.float32
    )


def staged(sep_rhs, matrix):
    f_local, sep_size, rhs_count = sep_rhs.shape

    def body(rhs_ref, matrix_ref, out_ref, held_ref):
        for f in range(f_local):
            for s in range(0, sep_size, TILE):
                out_ref[f, :, s : s + TILE] = rhs_ref[f, s : s + TILE, :].astype(jnp.float32).T
                held_ref[f, s : s + TILE] = matrix_ref[f, s : s + TILE]

    return pl.pallas_call(
        body,
        in_specs=in_vmem(2),
        out_specs=in_vmem(2),
        out_shape=[
            jax.ShapeDtypeStruct((f_local, rhs_count, sep_size), jnp.float32),
            jax.ShapeDtypeStruct(matrix.shape, matrix.dtype),
        ],
        compiler_params=room(4),
        cost_estimate=cost(sep_rhs.size, sep_rhs.size * 6 + matrix.size * 4),
    )(sep_rhs, matrix)


def first_solve(rhs, parts, matrix):
    f_local, rhs_count, sep_size = rhs.shape

    def body(rhs_ref, *rest):
        parts_refs, (matrix_ref, right_ref, out_ref, sent_ref) = rest[:-4], rest[-4:]
        for f in range(f_local):
            right = rhs_ref[f]
            for part in parts_refs[SIDE * f : SIDE * f + SIDE]:
                right = right - part[...].astype(jnp.float32)
            right_ref[f] = right
            field = right.astype(jnp.bfloat16)
            for s in range(0, sep_size, TILE):
                out = across(field, matrix_ref[f, s : s + TILE])
                out_ref[f, :, s : s + TILE] = out
                sent_ref[f, :, s : s + TILE] = out.astype(jnp.bfloat16)

    return pl.pallas_call(
        body,
        in_specs=in_vmem(2 + len(parts)),
        out_specs=in_vmem(3),
        out_shape=[jax.ShapeDtypeStruct(rhs.shape, t) for t in (jnp.float32, jnp.float32, jnp.bfloat16)],
        compiler_params=room(8),
        cost_estimate=cost(2 * matrix.size * rhs_count, matrix.size * 2 + rhs.size * 24),
    )(rhs, *parts, matrix)


def residual_of(f, table_ref, right_ref, mine_ref, around_refs, coupling_ref):
    residual = right_ref[f] - mine_ref[f]
    for n, around in enumerate(around_refs):
        coupled = coupling_ref[f, pl.ds(table_ref[2 + n], 1), :]
        residual = residual + coupled * around[f].astype(jnp.float32)
    return residual


def sweep(table, right_side, mine, around, coupling, matrix):
    f_local, rhs_count, sep_size = mine.shape

    def body(table_ref, right_ref, mine_ref, *rest):
        around_refs, (coupling_ref, matrix_ref, out_ref, sent_ref) = rest[:4], rest[4:]
        for f in range(f_local):
            residual = residual_of(f, table_ref, right_ref, mine_ref, around_refs, coupling_ref)
            field = residual.astype(jnp.bfloat16)
            for s in range(0, sep_size, TILE):
                out = mine_ref[f, :, s : s + TILE] + across(field, matrix_ref[f, s : s + TILE])
                out_ref[f, :, s : s + TILE] = out
                sent_ref[f, :, s : s + TILE] = out.astype(jnp.bfloat16)

    return pl.pallas_call(
        body,
        in_specs=[pl.BlockSpec(memory_space=pltpu.MemorySpace.SMEM)] + in_vmem(8),
        out_specs=in_vmem(2),
        out_shape=[jax.ShapeDtypeStruct(mine.shape, t) for t in (jnp.float32, jnp.bfloat16)],
        compiler_params=room(8),
        cost_estimate=cost(2 * matrix.size * rhs_count, matrix.size * 2 + mine.size * 24),
    )(table, right_side, mine, *around, coupling, matrix)


def last_sweep(table, right_side, mine, around, coupling, matrix, copies):
    f_local, rhs_count, sep_size = mine.shape

    def body(table_ref, right_ref, mine_ref, *rest):
        around_refs, (coupling_ref, matrix_ref, out_ref, sum_ref) = rest[:4], rest[4:]
        total = 0.0
        for f in range(f_local):
            residual = residual_of(f, table_ref, right_ref, mine_ref, around_refs, coupling_ref)
            field = residual.astype(jnp.bfloat16)
            square = jnp.sum(residual * residual, axis=0, keepdims=True)
            total = total + square * table_ref[6 + f].astype(jnp.float32)
            for s in range(0, sep_size, TILE):
                step = across(matrix_ref[f, s : s + TILE], field)
                out_ref[f, s : s + TILE, :] = mine_ref[f, :, s : s + TILE].T + step
        sum_ref[...] = jnp.broadcast_to(jnp.sum(total), sum_ref.shape)

    return pl.pallas_call(
        body,
        in_specs=[pl.BlockSpec(memory_space=pltpu.MemorySpace.SMEM)] + in_vmem(8),
        out_specs=in_vmem(2),
        out_shape=[
            jax.ShapeDtypeStruct((f_local, sep_size, rhs_count), jnp.float32),
            jax.ShapeDtypeStruct((copies, 8, 128), jnp.float32),
        ],
        compiler_params=room(8),
        cost_estimate=cost(2 * matrix.size * rhs_count, matrix.size * 2 + mine.size * 24),
    )(table, right_side, mine, *around, coupling, matrix)


def turn(x, axis, by):
    return lax.ppermute(x, axis, [(i, (i + by) % SIDE) for i in range(SIDE)])


def neighbours(x, axis, count):
    pairs = [[(i, i + 1) for i in range(first, count - 1, 2)] for first in range(2)]
    return tuple(lax.ppermute(x, axis, p + [(b, a) for a, b in p]) for p in pairs)


def on_device(update_basis, update_coeff, owner, sep_rhs, coupling, frontal_inverse):
    f_local = update_basis.shape[0]
    sep_size = update_basis.shape[3]
    rhs_count = update_coeff.shape[3]
    columns, rows = lax.axis_size(SX), lax.axis_size("sy")
    odd = [lax.rem(lax.axis_index(axis).astype(jnp.int32), 2) for axis in (SX, "sy")]
    freq_ids = [lax.axis_index("freq").astype(jnp.int32) * f_local + f + 1 for f in range(f_local)]
    place = [lax.axis_index(axis).astype(jnp.int32) for axis in SX]
    rows_of = [1 - odd[0], odd[0], 3 - odd[1], 2 + odd[1]]
    table = jnp.stack(place + rows_of + [i * i for i in freq_ids])
    data = (owner[:, 0], table, update_basis, update_coeff)
    half, full = jnp.bfloat16, jnp.float32

    axes = (SX, SX[::-1])
    plan = tuple((2 * f + n, 0, f, 2, pair) for f in range(2) for n, pair in enumerate((LOW, HIGH)))
    far = owner_products(plan, ((2, half),) * 4, *data, fetched=True)
    got = [(turn(far[2 * f], axes[f][0], 1), turn(far[2 * f + 1], axes[f][0], -1)) for f in range(2)]

    sides = ((1, LOW, HIGH), (3, HIGH, LOW))
    plan = tuple(
        (4 * late + 2 * f + n, 2 * late, f, ahead, pairs[late])
        for f in range(2)
        for n, (ahead, *pairs) in enumerate(sides)
        for late in range(2)
    )
    near = owner_products(plan, ((2, full),) * 4 + ((4, half),) * 4, *data)

    sums, joined = [], []
    for f in range(2):
        following = join(near[2 * f], got[f][0], near[4 + 2 * f])
        preceding = join(near[2 * f + 1], got[f][1], near[5 + 2 * f])
        joined += [following, preceding]
        sums.append((turn(following, axes[f][0], 1), turn(preceding, axes[f][0], -1)))
    plan = tuple((f, 2 * n, f, 0, pair) for f in range(2) for n, pair in enumerate((LOW, HIGH)))
    own = owner_products(plan, ((4, full),) * 2, *data, after=tuple(joined))
    rhs, matrix = staged(sep_rhs[:, 0, 0], frontal_inverse[:, 0, 0])

    parts = []
    for f in range(2):
        here, following, preceding, opposite = row_totals(own[f], *sums[f])
        axis = axes[f][1]
        parts += [here, turn(opposite, axis, 2), turn(following, axis, 1), turn(preceding, axis, -1)]

    coupling_rows = coupling[:, 0, 0]
    right_side, mine, sent = first_solve(rhs, parts, matrix)
    for _ in range(SWEEPS - 1):
        around = neighbours(sent, SX, columns) + neighbours(sent, "sy", rows)
        mine, sent = sweep(table, right_side, mine, around, coupling_rows, matrix)
    around = neighbours(sent, SX, columns) + neighbours(sent, "sy", rows)
    group = ("sy", "freq")
    solution, squares = last_sweep(
        table, right_side, mine, around, coupling_rows, matrix, lax.axis_size(group)
    )
    squares = jnp.sum(lax.all_to_all(squares, group, 0, 0, tiled=True), axis=0)
    squares = jnp.broadcast_to(squares, (columns, *squares.shape))
    squares = jnp.sum(lax.all_to_all(squares, SX, 0, 0, tiled=True), axis=0)
    entries = float(f_local * lax.axis_size("freq") * columns * rows * sep_size * rhs_count)
    residual_total = jnp.sqrt(squares[0, 0] / entries + 1e-06)
    return (solution[:, None, None], residual_total)


def solution(mesh):
    finer = Mesh(
        mesh.devices.reshape(SIDE, SIDE, mesh.shape["sy"], mesh.shape["freq"]),
        ("sx_0", "sx_1", "sy", "freq"),
    )
    return jax.shard_map(
        on_device,
        mesh=finer,
        in_specs=(
            P("freq", SX_SY, None, None),
            P("freq", SX_SY, None, None),
            P(SX_SY, None),
            P("freq", SX, "sy", None, None),
            P("freq", SX, "sy", None, None),
            P("freq", SX, "sy", None, None),
        ),
        out_specs=(P("freq", SX, "sy", None, None), P()),
        check_vma=False,
    )
```

```python
import functools

import jax
import jax.numpy as jnp
from jax import lax
from jax.experimental import pallas as pl
from jax.experimental.pallas import tpu as pltpu
from jax.sharding import Mesh
from jax.sharding import PartitionSpec as P


SWEEPS = 2
SIDE = 4
CAP = 4
TILE = 256
SX = ("sx_0", "sx_1")
SX_SY = ("sx_0", "sx_1", "sy")
LOW, HIGH = (0, 1), (3, 2)


def cost(flops, bytes_accessed):
    return pl.CostEstimate(flops=flops, bytes_accessed=bytes_accessed, transcendentals=0)


def room(mebibytes):
    return pltpu.CompilerParams(vmem_limit_bytes=mebibytes << 20)


def fill_slots(owner_ref, slots, used):
    children = owner_ref.shape[0]
    for o in range(SIDE * SIDE):
        used[o] = 0
    for s in range(SIDE * SIDE * CAP):
        slots[s] = children

    def put(c, carry):
        o = owner_ref[c]
        k = used[o]
        slots[o * CAP + k] = c
        used[o] = k + 1
        return carry

    lax.fori_loop(0, children, put, 0)


def owner_at(table_ref, f, ahead, beside):
    offsets = (ahead, beside) if f == 0 else (beside, ahead)
    row = lax.rem(table_ref[0] + offsets[0], SIDE)
    column = lax.rem(table_ref[1] + offsets[1], SIDE)
    return row * SIDE + column


def multiply(weights, stacked, out, at):
    rhs_count = out.shape[1]
    turned = weights[...].T
    for s in range(0, stacked.shape[1], TILE):
        product = jnp.dot(turned, stacked[:, s : s + TILE], preferred_element_type=jnp.float32)
        for b in range(2):
            piece = product[b * rhs_count : (b + 1) * rhs_count]
            out[at + b, :, s : s + TILE] = piece.astype(out.dtype)


def put_weights(weights, coeff_ref, f, c, filled, b, k):
    rank, rhs_count = coeff_ref.shape[2:]
    at = (b * CAP + k) * rank
    coeff = coeff_ref[f, c]
    weights[at : at + rank, b * rhs_count : (b + 1) * rhs_count] = jnp.where(
        filled, coeff, jnp.zeros_like(coeff)
    )


def owner_products(plan, shapes, owners, place, basis, coeff, after=(), fetched=False):
    _, children, rank, sep_size = basis.shape
    rhs_count = coeff.shape[3]
    count = len(plan) if fetched else 1
    depth = 2 * CAP * rank

    def body(owner_ref, table_ref, basis_ref, coeff_ref, *rest):
        outs = rest[len(after) : len(after) + len(shapes)]
        slots, used, stacked, weights = rest[len(after) + len(shapes) :][:4]
        arrived = rest[-1]
        fill_slots(owner_ref, slots, used)

        def child(f, ahead, beside, k):
            c = slots[owner_at(table_ref, f, ahead, beside) * CAP + k]
            filled = c < children
            return jnp.where(filled, c, 0), filled

        def copies(n):
            _, _, f, ahead, pair = plan[n]
            return [
                pltpu.make_async_copy(
                    basis_ref.at[f, child(f, ahead, beside, k)[0]],
                    stacked.at[n, pl.ds((b * CAP + k) * rank, rank)],
                    arrived.at[n],
                )
                for b, beside in enumerate(pair)
                for k in range(CAP)
            ]

        if fetched:
            flights = [copies(n) for n in range(len(plan))]
            for flight in flights:
                for copy in flight:
                    copy.start()
        weights[...] = jnp.zeros_like(weights)
        for n, (out, at, f, ahead, pair) in enumerate(plan):
            for b, beside in enumerate(pair):
                for k in range(CAP):
                    c, filled = child(f, ahead, beside, k)
                    put_weights(weights, coeff_ref, f, c, filled, b, k)
                    if not fetched:
                        stacked[0, pl.ds((b * CAP + k) * rank, rank)] = basis_ref[f, c]
            if fetched:
                for copy in flights[n]:
                    copy.wait()
            multiply(weights, stacked.at[n if fetched else 0], outs[out], at)

    space = pltpu.MemorySpace.HBM if fetched else pltpu.MemorySpace.VMEM
    return pl.pallas_call(
        body,
        in_specs=[pl.BlockSpec(memory_space=pltpu.MemorySpace.SMEM)] * 2
        + [pl.BlockSpec(memory_space=space), pl.BlockSpec(memory_space=pltpu.MemorySpace.VMEM)]
        + [pl.BlockSpec(memory_space=pl.ANY) for _ in after],
        out_specs=[pl.BlockSpec(memory_space=pltpu.MemorySpace.VMEM) for _ in shapes],
        scratch_shapes=[
            pltpu.SMEM((SIDE * SIDE * CAP,), jnp.int32),
            pltpu.SMEM((SIDE * SIDE,), jnp.int32),
            pltpu.VMEM((count, depth, sep_size), jnp.bfloat16),
            pltpu.VMEM((depth, 2 * rhs_count), jnp.bfloat16),
            pltpu.SemaphoreType.DMA((count,)),
        ],
        out_shape=[jax.ShapeDtypeStruct((n, rhs_count, sep_size), dtype) for n, dtype in shapes],
        compiler_params=room(53 if fetched else 16),
        cost_estimate=cost(
            2 * len(plan) * 4 * CAP * rank * sep_size * rhs_count * 2,
            len(plan) * 2 * (CAP * rank * sep_size * 2 + rhs_count * sep_size * 4),
        ),
    )(owners, place, basis, coeff, *after)


def in_vmem(count):
    return [pl.BlockSpec(memory_space=pltpu.MemorySpace.VMEM)] * count


def join(mine, got, whole):
    def body(mine_ref, got_ref, whole_ref, out_ref):
        n = mine_ref.shape[0]
        out_ref[:n] = (mine_ref[...] + got_ref[...].astype(jnp.float32)).astype(out_ref.dtype)

    return pl.pallas_call(
        body,
        in_specs=in_vmem(3),
        out_specs=in_vmem(1)[0],
        out_shape=jax.ShapeDtypeStruct(whole.shape, whole.dtype),
        input_output_aliases={2: 0},
        compiler_params=room(4),
        cost_estimate=cost(mine.size * 2, mine.size * 8),
    )(mine, got, whole)


def row_totals(own, low, high):
    _, rhs_count, sep_size = own.shape

    def body(own_ref, low_ref, high_ref, *outs):
        for at, out in enumerate(outs):
            crossed = (at + 2) % SIDE
            total = own_ref[at] + low_ref[at].astype(jnp.float32) + high_ref[crossed].astype(jnp.float32)
            out[...] = total.astype(out.dtype)

    types = (jnp.float32,) * 3 + (jnp.bfloat16,)
    return pl.pallas_call(
        body,
        in_specs=in_vmem(3),
        out_specs=in_vmem(SIDE),
        out_shape=[jax.ShapeDtypeStruct((rhs_count, sep_size), dtype) for dtype in types],
        compiler_params=room(4),
        cost_estimate=cost(own.size * 2, own.size * 12),
    )(own, low, high)


def across(field, matrix_tile):
    return lax.dot_general(
        field, matrix_tile, (((1,), (1,)), ((), ())), preferred_element_type=jnp.float32
    )


def staged(sep_rhs, matrix):
    f_local, sep_size, rhs_count = sep_rhs.shape

    def body(rhs_ref, matrix_ref, out_ref, held_ref):
        for f in range(f_local):
            for s in range(0, sep_size, TILE):
                out_ref[f, :, s : s + TILE] = rhs_ref[f, s : s + TILE, :].astype(jnp.float32).T
                held_ref[f, s : s + TILE] = matrix_ref[f, s : s + TILE]

    return pl.pallas_call(
        body,
        in_specs=in_vmem(2),
        out_specs=in_vmem(2),
        out_shape=[
            jax.ShapeDtypeStruct((f_local, rhs_count, sep_size), jnp.float32),
            jax.ShapeDtypeStruct(matrix.shape, matrix.dtype),
        ],
        compiler_params=room(4),
        cost_estimate=cost(sep_rhs.size, sep_rhs.size * 6 + matrix.size * 4),
    )(sep_rhs, matrix)


def first_solve(rhs, parts, matrix):
    f_local, rhs_count, sep_size = rhs.shape

    def body(rhs_ref, *rest):
        parts_refs, (matrix_ref, right_ref, out_ref, sent_ref) = rest[:-4], rest[-4:]
        for f in range(f_local):
            right = rhs_ref[f]
            for part in parts_refs[SIDE * f : SIDE * f + SIDE]:
                right = right - part[...].astype(jnp.float32)
            right_ref[f] = right
            field = right.astype(jnp.bfloat16)
            for s in range(0, sep_size, TILE):
                out = across(field, matrix_ref[f, s : s + TILE])
                out_ref[f, :, s : s + TILE] = out
                sent_ref[f, :, s : s + TILE] = out.astype(jnp.bfloat16)

    return pl.pallas_call(
        body,
        in_specs=in_vmem(2 + len(parts)),
        out_specs=in_vmem(3),
        out_shape=[jax.ShapeDtypeStruct(rhs.shape, t) for t in (jnp.float32, jnp.float32, jnp.bfloat16)],
        compiler_params=room(8),
        cost_estimate=cost(2 * matrix.size * rhs_count, matrix.size * 2 + rhs.size * 24),
    )(rhs, *parts, matrix)


def residual_of(f, table_ref, right_ref, mine_ref, around_refs, coupling_ref):
    residual = right_ref[f] - mine_ref[f]
    for n, around in enumerate(around_refs):
        coupled = coupling_ref[f, pl.ds(table_ref[2 + n], 1), :]
        coupled = jnp.where(table_ref[6 + n] > 0, coupled, jnp.zeros_like(coupled))
        residual = residual + coupled * around[f].astype(jnp.float32)
    return residual


def sweep(table, right_side, mine, around, coupling, matrix):
    f_local, rhs_count, sep_size = mine.shape

    def body(table_ref, right_ref, mine_ref, *rest):
        around_refs, (coupling_ref, matrix_ref, out_ref, sent_ref) = rest[:4], rest[4:]
        for f in range(f_local):
            residual = residual_of(f, table_ref, right_ref, mine_ref, around_refs, coupling_ref)
            field = residual.astype(jnp.bfloat16)
            for s in range(0, sep_size, TILE):
                out = mine_ref[f, :, s : s + TILE] + across(field, matrix_ref[f, s : s + TILE])
                out_ref[f, :, s : s + TILE] = out
                sent_ref[f, :, s : s + TILE] = out.astype(jnp.bfloat16)

    return pl.pallas_call(
        body,
        in_specs=[pl.BlockSpec(memory_space=pltpu.MemorySpace.SMEM)] + in_vmem(8),
        out_specs=in_vmem(2),
        out_shape=[jax.ShapeDtypeStruct(mine.shape, t) for t in (jnp.float32, jnp.bfloat16)],
        compiler_params=room(8),
        cost_estimate=cost(2 * matrix.size * rhs_count, matrix.size * 2 + mine.size * 24),
    )(table, right_side, mine, *around, coupling, matrix)


def last_sweep(table, right_side, mine, around, coupling, matrix, copies):
    f_local, rhs_count, sep_size = mine.shape

    def body(table_ref, right_ref, mine_ref, *rest):
        around_refs, (coupling_ref, matrix_ref, out_ref, sum_ref) = rest[:4], rest[4:]
        total = 0.0
        for f in range(f_local):
            residual = residual_of(f, table_ref, right_ref, mine_ref, around_refs, coupling_ref)
            field = residual.astype(jnp.bfloat16)
            square = jnp.sum(residual * residual, axis=0, keepdims=True)
            total = total + square * table_ref[10 + f].astype(jnp.float32)
            for s in range(0, sep_size, TILE):
                step = across(matrix_ref[f, s : s + TILE], field)
                out_ref[f, s : s + TILE, :] = mine_ref[f, :, s : s + TILE].T + step
        sum_ref[...] = jnp.broadcast_to(jnp.sum(total), sum_ref.shape)

    return pl.pallas_call(
        body,
        in_specs=[pl.BlockSpec(memory_space=pltpu.MemorySpace.SMEM)] + in_vmem(8),
        out_specs=in_vmem(2),
        out_shape=[
            jax.ShapeDtypeStruct((f_local, sep_size, rhs_count), jnp.float32),
            jax.ShapeDtypeStruct((copies, 8, 128), jnp.float32),
        ],
        compiler_params=room(8),
        cost_estimate=cost(2 * matrix.size * rhs_count, matrix.size * 2 + mine.size * 24),
    )(table, right_side, mine, *around, coupling, matrix)


def turn(x, axis, by):
    return lax.ppermute(x, axis, [(i, (i + by) % SIDE) for i in range(SIDE)])


def neighbours(x, axis, count):
    pairs = [[(i, (i + 1) % count) for i in range(first, count, 2)] for first in range(2)]
    return tuple(lax.ppermute(x, axis, p + [(b, a) for a, b in p]) for p in pairs)


def on_device(update_basis, update_coeff, owner, sep_rhs, coupling, frontal_inverse):
    f_local = update_basis.shape[0]
    sep_size = update_basis.shape[3]
    rhs_count = update_coeff.shape[3]
    columns, rows = lax.axis_size(SX), lax.axis_size("sy")
    odd = [lax.rem(lax.axis_index(axis).astype(jnp.int32), 2) for axis in (SX, "sy")]
    freq_ids = [lax.axis_index("freq").astype(jnp.int32) * f_local + f + 1 for f in range(f_local)]
    place = [lax.axis_index(axis).astype(jnp.int32) for axis in SX]
    rows_of = [1 - odd[0], odd[0], 3 - odd[1], 2 + odd[1]]
    inside = []
    for axis, count in ((SX, columns), ("sy", rows)):
        at = lax.axis_index(axis)
        inside += [jnp.int32(1), ((at > 0) & (at < count - 1)).astype(jnp.int32)]
    table = jnp.stack(place + rows_of + inside + [i * i for i in freq_ids])
    data = (owner[:, 0], table, update_basis, update_coeff)
    half, full = jnp.bfloat16, jnp.float32

    axes = (SX, SX[::-1])
    plan = tuple((2 * f + n, 0, f, 2, pair) for f in range(2) for n, pair in enumerate((LOW, HIGH)))
    far = owner_products(plan, ((2, half),) * 4, *data, fetched=True)
    got = [(turn(far[2 * f], axes[f][0], 1), turn(far[2 * f + 1], axes[f][0], -1)) for f in range(2)]

    sides = ((1, LOW, HIGH), (3, HIGH, LOW))
    plan = tuple(
        (4 * late + 2 * f + n, 2 * late, f, ahead, pairs[late])
        for f in range(2)
        for n, (ahead, *pairs) in enumerate(sides)
        for late in range(2)
    )
    near = owner_products(plan, ((2, full),) * 4 + ((4, half),) * 4, *data)

    sums, joined = [], []
    for f in range(2):
        following = join(near[2 * f], got[f][0], near[4 + 2 * f])
        preceding = join(near[2 * f + 1], got[f][1], near[5 + 2 * f])
        joined += [following, preceding]
        sums.append((turn(following, axes[f][0], 1), turn(preceding, axes[f][0], -1)))
    plan = tuple((f, 2 * n, f, 0, pair) for f in range(2) for n, pair in enumerate((LOW, HIGH)))
    own = owner_products(plan, ((4, full),) * 2, *data, after=tuple(joined))
    rhs, matrix = staged(sep_rhs[:, 0, 0], frontal_inverse[:, 0, 0])

    parts = []
    for f in range(2):
        here, following, preceding, opposite = row_totals(own[f], *sums[f])
        axis = axes[f][1]
        parts += [here, turn(opposite, axis, 2), turn(following, axis, 1), turn(preceding, axis, -1)]

    coupling_rows = coupling[:, 0, 0]
    right_side, mine, sent = first_solve(rhs, parts, matrix)
    for _ in range(SWEEPS - 1):
        around = neighbours(sent, SX, columns) + neighbours(sent, "sy", rows)
        mine, sent = sweep(table, right_side, mine, around, coupling_rows, matrix)
    around = neighbours(sent, SX, columns) + neighbours(sent, "sy", rows)
    group = ("sy", "freq")
    solution, squares = last_sweep(
        table, right_side, mine, around, coupling_rows, matrix, lax.axis_size(group)
    )
    squares = jnp.sum(lax.all_to_all(squares, group, 0, 0, tiled=True), axis=0)
    squares = jnp.broadcast_to(squares, (columns, *squares.shape))
    squares = jnp.sum(lax.all_to_all(squares, SX, 0, 0, tiled=True), axis=0)
    entries = float(f_local * lax.axis_size("freq") * columns * rows * sep_size * rhs_count)
    residual_total = jnp.sqrt(squares[0, 0] / entries + 1e-06)
    return (solution[:, None, None], residual_total)


def solution(mesh):
    finer = Mesh(
        mesh.devices.reshape(SIDE, SIDE, mesh.shape["sy"], mesh.shape["freq"]),
        ("sx_0", "sx_1", "sy", "freq"),
    )
    return jax.shard_map(
        on_device,
        mesh=finer,
        in_specs=(
            P("freq", SX_SY, None, None),
            P("freq", SX_SY, None, None),
            P(SX_SY, None),
            P("freq", SX, "sy", None, None),
            P("freq", SX, "sy", None, None),
            P("freq", SX, "sy", None, None),
        ),
        out_specs=(P("freq", SX, "sy", None, None), P()),
        check_vma=False,
    )
```

```python
import jax
import jax.numpy as jnp
from jax import lax
from jax.experimental import pallas as pl
from jax.experimental.pallas import tpu as pltpu
from jax.sharding import Mesh
from jax.sharding import PartitionSpec as P


SWEEPS = 2
SIDE = 4
CAP = 4
TILE = 256
SX = ("sx_0", "sx_1")
SX_SY = ("sx_0", "sx_1", "sy")
LOW, HIGH = (0, 1), (3, 2)


def cost(flops, bytes_accessed):
    return pl.CostEstimate(flops=flops, bytes_accessed=bytes_accessed, transcendentals=0)


def room(mebibytes):
    return pltpu.CompilerParams(vmem_limit_bytes=mebibytes << 20)


def fill_slots(owner_ref, slots, used):
    children = owner_ref.shape[0]
    for o in range(SIDE * SIDE):
        used[o] = 0
    for s in range(SIDE * SIDE * CAP):
        slots[s] = children

    def put(c, carry):
        o = owner_ref[c]
        k = used[o]
        slots[o * CAP + k] = c
        used[o] = k + 1
        return carry

    lax.fori_loop(0, children, put, 0)


def owner_at(table_ref, f, ahead, beside):
    offsets = (ahead, beside) if f == 0 else (beside, ahead)
    row = lax.rem(table_ref[0] + offsets[0], SIDE)
    column = lax.rem(table_ref[1] + offsets[1], SIDE)
    return row * SIDE + column


def multiply(weights, stacked, out, at):
    rhs_count = out.shape[1]
    turned = weights[...].T
    for s in range(0, stacked.shape[1], TILE):
        product = jnp.dot(turned, stacked[:, s : s + TILE], preferred_element_type=jnp.float32)
        for b in range(2):
            piece = product[b * rhs_count : (b + 1) * rhs_count]
            out[at + b, :, s : s + TILE] = piece.astype(out.dtype)


def put_weights(weights, coeff_ref, f, c, filled, b, k):
    rank, rhs_count = coeff_ref.shape[2:]
    at = (b * CAP + k) * rank
    coeff = coeff_ref[f, c]
    weights[at : at + rank, b * rhs_count : (b + 1) * rhs_count] = jnp.where(
        filled, coeff, jnp.zeros_like(coeff)
    )


def owner_products(plan, shapes, owners, place, basis, coeff, after=(), fetched=False):
    _, children, rank, sep_size = basis.shape
    rhs_count = coeff.shape[3]
    count = len(plan) if fetched else 1
    depth = 2 * CAP * rank

    def body(owner_ref, table_ref, basis_ref, coeff_ref, *rest):
        outs = rest[len(after) : len(after) + len(shapes)]
        slots, used, stacked, weights = rest[len(after) + len(shapes) :][:4]
        arrived = rest[-1]
        fill_slots(owner_ref, slots, used)

        def child(f, ahead, beside, k):
            c = slots[owner_at(table_ref, f, ahead, beside) * CAP + k]
            filled = c < children
            return jnp.where(filled, c, 0), filled

        def copies(n):
            _, _, f, ahead, pair = plan[n]
            return [
                pltpu.make_async_copy(
                    basis_ref.at[f, child(f, ahead, beside, k)[0]],
                    stacked.at[n, pl.ds((b * CAP + k) * rank, rank)],
                    arrived.at[n],
                )
                for b, beside in enumerate(pair)
                for k in range(CAP)
            ]

        if fetched:
            flights = [copies(n) for n in range(len(plan))]
            for flight in flights:
                for copy in flight:
                    copy.start()
        weights[...] = jnp.zeros_like(weights)
        for n, (out, at, f, ahead, pair) in enumerate(plan):
            for b, beside in enumerate(pair):
                for k in range(CAP):
                    c, filled = child(f, ahead, beside, k)
                    put_weights(weights, coeff_ref, f, c, filled, b, k)
                    if not fetched:
                        stacked[0, pl.ds((b * CAP + k) * rank, rank)] = basis_ref[f, c]
            if fetched:
                for copy in flights[n]:
                    copy.wait()
            multiply(weights, stacked.at[n if fetched else 0], outs[out], at)

    space = pltpu.MemorySpace.HBM if fetched else pltpu.MemorySpace.VMEM
    return pl.pallas_call(
        body,
        in_specs=[pl.BlockSpec(memory_space=pltpu.MemorySpace.SMEM)] * 2
        + [pl.BlockSpec(memory_space=space), pl.BlockSpec(memory_space=pltpu.MemorySpace.VMEM)]
        + [pl.BlockSpec(memory_space=pl.ANY) for _ in after],
        out_specs=[pl.BlockSpec(memory_space=pltpu.MemorySpace.VMEM) for _ in shapes],
        scratch_shapes=[
            pltpu.SMEM((SIDE * SIDE * CAP,), jnp.int32),
            pltpu.SMEM((SIDE * SIDE,), jnp.int32),
            pltpu.VMEM((count, depth, sep_size), jnp.bfloat16),
            pltpu.VMEM((depth, 2 * rhs_count), jnp.bfloat16),
            pltpu.SemaphoreType.DMA((count,)),
        ],
        out_shape=[jax.ShapeDtypeStruct((n, rhs_count, sep_size), dtype) for n, dtype in shapes],
        compiler_params=room(53 if fetched else 16),
        cost_estimate=cost(
            2 * len(plan) * 4 * CAP * rank * sep_size * rhs_count * 2,
            len(plan) * 2 * (CAP * rank * sep_size * 2 + rhs_count * sep_size * 4),
        ),
    )(owners, place, basis, coeff, *after)


def in_vmem(count):
    return [pl.BlockSpec(memory_space=pltpu.MemorySpace.VMEM)] * count


def join(mine, got, whole):
    def body(mine_ref, got_ref, whole_ref, out_ref):
        n = mine_ref.shape[0]
        out_ref[:n] = (mine_ref[...] + got_ref[...].astype(jnp.float32)).astype(out_ref.dtype)

    return pl.pallas_call(
        body,
        in_specs=in_vmem(3),
        out_specs=in_vmem(1)[0],
        out_shape=jax.ShapeDtypeStruct(whole.shape, whole.dtype),
        input_output_aliases={2: 0},
        compiler_params=room(4),
        cost_estimate=cost(mine.size * 2, mine.size * 8),
    )(mine, got, whole)


def row_totals(own, low, high):
    _, rhs_count, sep_size = own.shape

    def body(own_ref, low_ref, high_ref, *outs):
        for at, out in enumerate(outs):
            crossed = (at + 2) % SIDE
            total = own_ref[at] + low_ref[at].astype(jnp.float32) + high_ref[crossed].astype(jnp.float32)
            out[...] = total.astype(out.dtype)

    types = (jnp.float32,) * 3 + (jnp.bfloat16,)
    return pl.pallas_call(
        body,
        in_specs=in_vmem(3),
        out_specs=in_vmem(SIDE),
        out_shape=[jax.ShapeDtypeStruct((rhs_count, sep_size), dtype) for dtype in types],
        compiler_params=room(4),
        cost_estimate=cost(own.size * 2, own.size * 12),
    )(own, low, high)


def across(field, matrix_tile):
    return lax.dot_general(
        field, matrix_tile, (((1,), (1,)), ((), ())), preferred_element_type=jnp.float32
    )


def staged(sep_rhs, matrix):
    f_local, sep_size, rhs_count = sep_rhs.shape

    def body(rhs_ref, matrix_ref, out_ref, held_ref):
        for f in range(f_local):
            for s in range(0, sep_size, TILE):
                out_ref[f, :, s : s + TILE] = rhs_ref[f, s : s + TILE, :].astype(jnp.float32).T
                held_ref[f, s : s + TILE] = matrix_ref[f, s : s + TILE]

    return pl.pallas_call(
        body,
        in_specs=in_vmem(2),
        out_specs=in_vmem(2),
        out_shape=[
            jax.ShapeDtypeStruct((f_local, rhs_count, sep_size), jnp.float32),
            jax.ShapeDtypeStruct(matrix.shape, matrix.dtype),
        ],
        compiler_params=room(4),
        cost_estimate=cost(sep_rhs.size, sep_rhs.size * 6 + matrix.size * 4),
    )(sep_rhs, matrix)


def solve_cost(rhs_count, sep_size):
    return cost(2 * sep_size * sep_size * rhs_count, sep_size * (2 * sep_size + 24 * rhs_count))


def first_solve(f, rhs, parts, matrix):
    _, rhs_count, sep_size = rhs.shape

    def body(rhs_ref, *rest):
        parts_refs, (matrix_ref, right_ref, out_ref, sent_ref) = rest[:-4], rest[-4:]
        right = rhs_ref[f]
        for part in parts_refs:
            right = right - part[...].astype(jnp.float32)
        right_ref[...] = right
        field = right.astype(jnp.bfloat16)
        for s in range(0, sep_size, TILE):
            out = across(field, matrix_ref[f, s : s + TILE])
            out_ref[:, s : s + TILE] = out
            sent_ref[:, s : s + TILE] = out.astype(jnp.bfloat16)

    types = (jnp.float32, jnp.float32, jnp.bfloat16)
    return pl.pallas_call(
        body,
        in_specs=in_vmem(2 + len(parts)),
        out_specs=in_vmem(3),
        out_shape=[jax.ShapeDtypeStruct((rhs_count, sep_size), t) for t in types],
        compiler_params=room(6),
        cost_estimate=solve_cost(rhs_count, sep_size),
    )(rhs, *parts, matrix)


def residual_of(f, table_ref, right_ref, mine_ref, around_refs, coupling_ref):
    residual = right_ref[...] - mine_ref[...]
    for n, around in enumerate(around_refs):
        coupled = coupling_ref[f, pl.ds(table_ref[2 + n], 1), :]
        coupled = jnp.where(table_ref[6 + n] > 0, coupled, jnp.zeros_like(coupled))
        residual = residual + coupled * around[...].astype(jnp.float32)
    return residual


def sweep(f, table, right_side, mine, around, coupling, matrix):
    rhs_count, sep_size = mine.shape

    def body(table_ref, right_ref, mine_ref, *rest):
        around_refs, (coupling_ref, matrix_ref, out_ref, sent_ref) = rest[:4], rest[4:]
        residual = residual_of(f, table_ref, right_ref, mine_ref, around_refs, coupling_ref)
        field = residual.astype(jnp.bfloat16)
        for s in range(0, sep_size, TILE):
            out = mine_ref[:, s : s + TILE] + across(field, matrix_ref[f, s : s + TILE])
            out_ref[:, s : s + TILE] = out
            sent_ref[:, s : s + TILE] = out.astype(jnp.bfloat16)

    return pl.pallas_call(
        body,
        in_specs=[pl.BlockSpec(memory_space=pltpu.MemorySpace.SMEM)] + in_vmem(8),
        out_specs=in_vmem(2),
        out_shape=[jax.ShapeDtypeStruct(mine.shape, t) for t in (jnp.float32, jnp.bfloat16)],
        compiler_params=room(6),
        cost_estimate=solve_cost(rhs_count, sep_size),
    )(table, right_side, mine, *around, coupling, matrix)


def last_sweep(f, table, right_side, mine, around, coupling, matrix, before, copies):
    rhs_count, sep_size = mine.shape
    f_local = matrix.shape[0]

    def body(table_ref, right_ref, mine_ref, *rest):
        around_refs, (coupling_ref, matrix_ref), rest = rest[:4], rest[4:6], rest[6:]
        out_ref, sum_ref = rest[len(before) :]
        residual = residual_of(f, table_ref, right_ref, mine_ref, around_refs, coupling_ref)
        field = residual.astype(jnp.bfloat16)
        square = jnp.sum(residual * residual, axis=0, keepdims=True)
        total = jnp.sum(square * table_ref[10 + f].astype(jnp.float32))
        total = jnp.broadcast_to(total, sum_ref.shape)
        sum_ref[...] = total + rest[1][...] if before else total
        for s in range(0, sep_size, TILE):
            step = across(matrix_ref[f, s : s + TILE], field)
            out_ref[0, s : s + TILE, :] = mine_ref[:, s : s + TILE].T + step

    return pl.pallas_call(
        body,
        grid=(1,),
        in_specs=[pl.BlockSpec(memory_space=pltpu.MemorySpace.SMEM)]
        + in_vmem(8)
        + ([pl.BlockSpec(memory_space=pl.ANY)] + in_vmem(1) if before else []),
        out_specs=[pl.BlockSpec((1, sep_size, rhs_count), lambda i: (f, 0, 0)), in_vmem(1)[0]],
        out_shape=[
            jax.ShapeDtypeStruct((f_local, sep_size, rhs_count), jnp.float32),
            jax.ShapeDtypeStruct((copies, 8, 128), jnp.float32),
        ],
        input_output_aliases={9: 0} if before else {},
        compiler_params=room(6),
        cost_estimate=solve_cost(rhs_count, sep_size),
    )(table, right_side, mine, *around, coupling, matrix, *before)


def turn(x, axis, by):
    return lax.ppermute(x, axis, [(i, (i + by) % SIDE) for i in range(SIDE)])


def neighbours(x, axis, count):
    pairs = [[(i, (i + 1) % count) for i in range(first, count, 2)] for first in range(2)]
    return tuple(lax.ppermute(x, axis, p + [(b, a) for a, b in p]) for p in pairs)


def on_device(update_basis, update_coeff, owner, sep_rhs, coupling, frontal_inverse):
    f_local = update_basis.shape[0]
    sep_size = update_basis.shape[3]
    rhs_count = update_coeff.shape[3]
    columns, rows = lax.axis_size(SX), lax.axis_size("sy")
    odd = [lax.rem(lax.axis_index(axis).astype(jnp.int32), 2) for axis in (SX, "sy")]
    freq_ids = [lax.axis_index("freq").astype(jnp.int32) * f_local + f + 1 for f in range(f_local)]
    place = [lax.axis_index(axis).astype(jnp.int32) for axis in SX]
    rows_of = [1 - odd[0], odd[0], 3 - odd[1], 2 + odd[1]]
    inside = []
    for axis, count in ((SX, columns), ("sy", rows)):
        at = lax.axis_index(axis)
        inside += [jnp.int32(1), ((at > 0) & (at < count - 1)).astype(jnp.int32)]
    table = jnp.stack(place + rows_of + inside + [i * i for i in freq_ids])
    data = (owner[:, 0], table, update_basis, update_coeff)
    half, full = jnp.bfloat16, jnp.float32

    axes = (SX, SX[::-1])
    plan = tuple((2 * f + n, 0, f, 2, pair) for f in range(2) for n, pair in enumerate((LOW, HIGH)))
    far = owner_products(plan, ((2, half),) * 4, *data, fetched=True)
    got = [(turn(far[2 * f], axes[f][0], 1), turn(far[2 * f + 1], axes[f][0], -1)) for f in range(2)]

    sides = ((1, LOW, HIGH), (3, HIGH, LOW))
    plan = tuple(
        (4 * late + 2 * f + n, 2 * late, f, ahead, pairs[late])
        for f in range(2)
        for n, (ahead, *pairs) in enumerate(sides)
        for late in range(2)
    )
    near = owner_products(plan, ((2, full),) * 4 + ((4, half),) * 4, *data)

    sums, joined = [], []
    for f in range(2):
        following = join(near[2 * f], got[f][0], near[4 + 2 * f])
        preceding = join(near[2 * f + 1], got[f][1], near[5 + 2 * f])
        joined += [following, preceding]
        sums.append((turn(following, axes[f][0], 1), turn(preceding, axes[f][0], -1)))
    plan = tuple((f, 2 * n, f, 0, pair) for f in range(2) for n, pair in enumerate((LOW, HIGH)))
    own = owner_products(plan, ((4, full),) * 2, *data, after=tuple(joined))
    rhs, matrix = staged(sep_rhs[:, 0, 0], frontal_inverse[:, 0, 0])

    coupling_rows = coupling[:, 0, 0]
    order = (1, 0)
    right_side, mine, sent = {}, {}, {}
    for f in order:
        here, following, preceding, opposite = row_totals(own[f], *sums[f])
        axis = axes[f][1]
        opposite = turn(opposite, axis, 2)
        parts = (opposite, turn(following, axis, 1), turn(preceding, axis, -1))
        right_side[f], mine[f], sent[f] = first_solve(f, rhs, (here, *parts), matrix)
    for _ in range(SWEEPS - 1):
        for f in order:
            around = neighbours(sent[f], SX, columns) + neighbours(sent[f], "sy", rows)
            mine[f], sent[f] = sweep(f, table, right_side[f], mine[f], around, coupling_rows, matrix)
    group = ("sy", "freq")
    done = ()
    for f in order:
        around = neighbours(sent[f], SX, columns) + neighbours(sent[f], "sy", rows)
        done = last_sweep(
            f, table, right_side[f], mine[f], around, coupling_rows, matrix, done, lax.axis_size(group)
        )
    solution, squares = done
    squares = jnp.sum(lax.all_to_all(squares, group, 0, 0, tiled=True), axis=0)
    squares = jnp.broadcast_to(squares, (columns, *squares.shape))
    squares = jnp.sum(lax.all_to_all(squares, SX, 0, 0, tiled=True), axis=0)
    entries = float(f_local * lax.axis_size("freq") * columns * rows * sep_size * rhs_count)
    residual_total = jnp.sqrt(squares[0, 0] / entries + 1e-06)
    return (solution[:, None, None], residual_total)


def solution(mesh):
    finer = Mesh(
        mesh.devices.reshape(SIDE, SIDE, mesh.shape["sy"], mesh.shape["freq"]),
        ("sx_0", "sx_1", "sy", "freq"),
    )

    return jax.shard_map(
        on_device,
        mesh=finer,
        in_specs=(
            P("freq", SX_SY, None, None),
            P("freq", SX_SY, None, None),
            P(SX_SY, None),
            P("freq", SX, "sy", None, None),
            P("freq", SX, "sy", None, None),
            P("freq", SX, "sy", None, None),
        ),
        out_specs=(P("freq", SX, "sy", None, None), P()),
        check_vma=False,
    )
```

```python
import jax
import jax.numpy as jnp
from jax import lax
from jax.experimental import pallas as pl
from jax.experimental.pallas import tpu as pltpu
from jax.sharding import Mesh
from jax.sharding import PartitionSpec as P


SWEEPS = 2
SIDE = 4
CAP = 4
TILE = 256
SPARE = 16
SX = ("sx_0", "sx_1")
SX_SY = ("sx_0", "sx_1", "sy")
LOW, HIGH = (0, 1), (3, 2)


def cost(flops, bytes_accessed):
    return pl.CostEstimate(flops=flops, bytes_accessed=bytes_accessed, transcendentals=0)


def room(mebibytes):
    return pltpu.CompilerParams(vmem_limit_bytes=mebibytes << 20)


def fill_slots(owner_ref, slots, used):
    children = owner_ref.shape[0]
    for o in range(SIDE * SIDE):
        used[o] = 0
    for s in range(SIDE * SIDE * CAP):
        slots[s] = children

    def put(c, carry):
        o = owner_ref[c]
        k = used[o]
        slots[o * CAP + k] = c
        used[o] = k + 1
        return carry

    lax.fori_loop(0, children, put, 0)


def owner_at(table_ref, f, ahead, beside):
    offsets = (ahead, beside) if f == 0 else (beside, ahead)
    row = lax.rem(table_ref[0] + offsets[0], SIDE)
    column = lax.rem(table_ref[1] + offsets[1], SIDE)
    return row * SIDE + column


def multiply(weights, stacked, out, at):
    rhs_count = out.shape[1]
    turned = weights[...].T
    for s in range(0, stacked.shape[1], TILE):
        product = jnp.dot(turned, stacked[:, s : s + TILE], preferred_element_type=jnp.float32)
        for b in range(2):
            piece = product[b * rhs_count : (b + 1) * rhs_count]
            out[at + b, :, s : s + TILE] = piece.astype(out.dtype)


def put_weights(weights, coeff_ref, f, c, filled, b, k):
    rank, rhs_count = coeff_ref.shape[2:]
    at = (b * CAP + k) * rank
    coeff = coeff_ref[f, c]
    weights[at : at + rank, b * rhs_count : (b + 1) * rhs_count] = jnp.where(
        filled, coeff, jnp.zeros_like(coeff)
    )


def owner_products(plan, shapes, owners, place, basis, coeff, after=(), fetched=False):
    _, children, rank, sep_size = basis.shape
    rhs_count = coeff.shape[3]
    count = len(plan) if fetched else 1
    depth = 2 * CAP * rank

    def body(owner_ref, table_ref, basis_ref, coeff_ref, *rest):
        outs = rest[len(after) : len(after) + len(shapes)]
        slots, used, stacked, weights = rest[len(after) + len(shapes) :][:4]
        arrived = rest[-1]
        fill_slots(owner_ref, slots, used)

        def child(f, ahead, beside, k):
            c = slots[owner_at(table_ref, f, ahead, beside) * CAP + k]
            filled = c < children
            return jnp.where(filled, c, 0), filled

        def copies(n):
            _, _, f, ahead, pair = plan[n]
            return [
                pltpu.make_async_copy(
                    basis_ref.at[f, child(f, ahead, beside, k)[0]],
                    stacked.at[n, pl.ds((b * CAP + k) * rank, rank)],
                    arrived.at[n],
                )
                for b, beside in enumerate(pair)
                for k in range(CAP)
            ]

        if fetched:
            flights = [copies(n) for n in range(len(plan))]
            for flight in flights:
                for copy in flight:
                    copy.start()
        weights[...] = jnp.zeros_like(weights)
        for n, (out, at, f, ahead, pair) in enumerate(plan):
            for b, beside in enumerate(pair):
                for k in range(CAP):
                    c, filled = child(f, ahead, beside, k)
                    put_weights(weights, coeff_ref, f, c, filled, b, k)
                    if not fetched:
                        stacked[0, pl.ds((b * CAP + k) * rank, rank)] = basis_ref[f, c]
            if fetched:
                for copy in flights[n]:
                    copy.wait()
            multiply(weights, stacked.at[n if fetched else 0], outs[out], at)

    space = pltpu.MemorySpace.HBM if fetched else pltpu.MemorySpace.VMEM
    return pl.pallas_call(
        body,
        in_specs=[pl.BlockSpec(memory_space=pltpu.MemorySpace.SMEM)] * 2
        + [pl.BlockSpec(memory_space=space), pl.BlockSpec(memory_space=pltpu.MemorySpace.VMEM)]
        + [pl.BlockSpec(memory_space=pl.ANY) for _ in after],
        out_specs=[pl.BlockSpec(memory_space=pltpu.MemorySpace.VMEM) for _ in shapes],
        scratch_shapes=[
            pltpu.SMEM((SIDE * SIDE * CAP,), jnp.int32),
            pltpu.SMEM((SIDE * SIDE,), jnp.int32),
            pltpu.VMEM((count, depth, sep_size), jnp.bfloat16),
            pltpu.VMEM((depth, 2 * rhs_count), jnp.bfloat16),
            pltpu.SemaphoreType.DMA((count,)),
        ],
        out_shape=[jax.ShapeDtypeStruct((n, rhs_count, sep_size), dtype) for n, dtype in shapes],
        compiler_params=room(53 if fetched else 16),
        cost_estimate=cost(
            2 * len(plan) * 4 * CAP * rank * sep_size * rhs_count * 2,
            len(plan) * 2 * (CAP * rank * sep_size * 2 + rhs_count * sep_size * 4),
        ),
    )(owners, place, basis, coeff, *after)


def in_vmem(count):
    return [pl.BlockSpec(memory_space=pltpu.MemorySpace.VMEM)] * count


def join(mine, got, whole):
    def body(mine_ref, got_ref, whole_ref, out_ref):
        n = mine_ref.shape[0]
        out_ref[:n] = (mine_ref[...] + got_ref[...].astype(jnp.float32)).astype(out_ref.dtype)

    return pl.pallas_call(
        body,
        in_specs=in_vmem(3),
        out_specs=in_vmem(1)[0],
        out_shape=jax.ShapeDtypeStruct(whole.shape, whole.dtype),
        input_output_aliases={2: 0},
        compiler_params=room(4),
        cost_estimate=cost(mine.size * 2, mine.size * 8),
    )(mine, got, whole)


def row_totals(own, low, high):
    _, rhs_count, sep_size = own.shape

    def body(own_ref, low_ref, high_ref, here, following, preceding, opposite):
        def total(at):
            crossed = (at + 2) % SIDE
            return own_ref[at] + low_ref[at].astype(jnp.float32) + high_ref[crossed].astype(jnp.float32)

        here[...] = total(0)
        for at, out in ((1, following), (2, preceding)):
            sums = total(at)
            largest = jnp.max(jnp.abs(sums), axis=0, keepdims=True)
            largest = jnp.broadcast_to(jnp.max(largest), (SPARE, sep_size))
            power = jnp.clip(14.0 - jnp.ceil(jnp.log2(largest)), -60.0, 100.0)
            out[:rhs_count] = sums * jnp.exp2(power[:1])
            out[rhs_count:] = power
        opposite[...] = total(3).astype(jnp.bfloat16)

    plain = (rhs_count, sep_size)
    wide = (rhs_count + SPARE, sep_size)
    return pl.pallas_call(
        body,
        in_specs=in_vmem(3),
        out_specs=in_vmem(SIDE),
        out_shape=[jax.ShapeDtypeStruct(shape, jnp.float32) for shape in (plain, wide, wide)]
        + [jax.ShapeDtypeStruct(plain, jnp.bfloat16)],
        compiler_params=room(4),
        cost_estimate=cost(own.size * 2, own.size * 12),
    )(own, low, high)


def across(field, matrix_tile):
    return lax.dot_general(
        field, matrix_tile, (((1,), (1,)), ((), ())), preferred_element_type=jnp.float32
    )


def staged(sep_rhs, matrix):
    f_local, sep_size, rhs_count = sep_rhs.shape

    def body(rhs_ref, matrix_ref, out_ref, held_ref):
        for f in range(f_local):
            for s in range(0, sep_size, TILE):
                out_ref[f, :, s : s + TILE] = rhs_ref[f, s : s + TILE, :].astype(jnp.float32).T
                held_ref[f, s : s + TILE] = matrix_ref[f, s : s + TILE]

    return pl.pallas_call(
        body,
        in_specs=in_vmem(2),
        out_specs=in_vmem(2),
        out_shape=[
            jax.ShapeDtypeStruct((f_local, rhs_count, sep_size), jnp.float32),
            jax.ShapeDtypeStruct(matrix.shape, matrix.dtype),
        ],
        compiler_params=room(4),
        cost_estimate=cost(sep_rhs.size, sep_rhs.size * 6 + matrix.size * 4),
    )(sep_rhs, matrix)


def solve_cost(rhs_count, sep_size):
    return cost(2 * sep_size * sep_size * rhs_count, sep_size * (2 * sep_size + 24 * rhs_count))


def first_solve(f, rhs, parts, matrix):
    _, rhs_count, sep_size = rhs.shape

    def body(rhs_ref, *rest):
        parts_refs, (matrix_ref, right_ref, out_ref, sent_ref) = rest[:-4], rest[-4:]
        here, opposite, *beside = parts_refs
        right = rhs_ref[f] - here[...] - opposite[...].astype(jnp.float32)
        for part in beside:
            right = right - part[:rhs_count] * jnp.exp2(-part[rhs_count : rhs_count + 1])
        right_ref[...] = right
        field = right.astype(jnp.bfloat16)
        for s in range(0, sep_size, TILE):
            out = across(field, matrix_ref[f, s : s + TILE])
            out_ref[:, s : s + TILE] = out
            sent_ref[:, s : s + TILE] = out.astype(jnp.bfloat16)

    types = (jnp.float32, jnp.float32, jnp.bfloat16)
    return pl.pallas_call(
        body,
        in_specs=in_vmem(2 + len(parts)),
        out_specs=in_vmem(3),
        out_shape=[jax.ShapeDtypeStruct((rhs_count, sep_size), t) for t in types],
        compiler_params=room(6),
        cost_estimate=solve_cost(rhs_count, sep_size),
    )(rhs, *parts, matrix)


def residual_of(f, table_ref, right_ref, mine_ref, around_refs, coupling_ref):
    residual = right_ref[...] - mine_ref[...]
    for n, around in enumerate(around_refs):
        coupled = coupling_ref[f, pl.ds(table_ref[2 + n], 1), :]
        coupled = jnp.where(table_ref[6 + n] > 0, coupled, jnp.zeros_like(coupled))
        residual = residual + coupled * around[...].astype(jnp.float32)
    return residual


def sweep(f, table, right_side, mine, around, coupling, matrix):
    rhs_count, sep_size = mine.shape

    def body(table_ref, right_ref, mine_ref, *rest):
        around_refs, (coupling_ref, matrix_ref, out_ref, sent_ref) = rest[:4], rest[4:]
        residual = residual_of(f, table_ref, right_ref, mine_ref, around_refs, coupling_ref)
        field = residual.astype(jnp.bfloat16)
        for s in range(0, sep_size, TILE):
            out = mine_ref[:, s : s + TILE] + across(field, matrix_ref[f, s : s + TILE])
            out_ref[:, s : s + TILE] = out
            sent_ref[:, s : s + TILE] = out.astype(jnp.bfloat16)

    return pl.pallas_call(
        body,
        in_specs=[pl.BlockSpec(memory_space=pltpu.MemorySpace.SMEM)] + in_vmem(8),
        out_specs=in_vmem(2),
        out_shape=[jax.ShapeDtypeStruct(mine.shape, t) for t in (jnp.float32, jnp.bfloat16)],
        compiler_params=room(6),
        cost_estimate=solve_cost(rhs_count, sep_size),
    )(table, right_side, mine, *around, coupling, matrix)


def last_sweep(f, table, right_side, mine, around, coupling, matrix, before, copies):
    rhs_count, sep_size = mine.shape
    f_local = matrix.shape[0]

    def body(table_ref, right_ref, mine_ref, *rest):
        around_refs, (coupling_ref, matrix_ref), rest = rest[:4], rest[4:6], rest[6:]
        out_ref, sum_ref = rest[len(before) :]
        residual = residual_of(f, table_ref, right_ref, mine_ref, around_refs, coupling_ref)
        field = residual.astype(jnp.bfloat16)
        square = jnp.sum(residual * residual, axis=0, keepdims=True)
        total = jnp.sum(square * table_ref[10 + f].astype(jnp.float32))
        total = jnp.broadcast_to(total, sum_ref.shape)
        sum_ref[...] = total + rest[1][...] if before else total
        for s in range(0, sep_size, TILE):
            step = across(matrix_ref[f, s : s + TILE], field)
            out_ref[0, s : s + TILE, :] = mine_ref[:, s : s + TILE].T + step

    return pl.pallas_call(
        body,
        grid=(1,),
        in_specs=[pl.BlockSpec(memory_space=pltpu.MemorySpace.SMEM)]
        + in_vmem(8)
        + ([pl.BlockSpec(memory_space=pl.ANY)] + in_vmem(1) if before else []),
        out_specs=[pl.BlockSpec((1, sep_size, rhs_count), lambda i: (f, 0, 0)), in_vmem(1)[0]],
        out_shape=[
            jax.ShapeDtypeStruct((f_local, sep_size, rhs_count), jnp.float32),
            jax.ShapeDtypeStruct((copies, 8, 128), jnp.float32),
        ],
        input_output_aliases={9: 0} if before else {},
        compiler_params=room(6),
        cost_estimate=solve_cost(rhs_count, sep_size),
    )(table, right_side, mine, *around, coupling, matrix, *before)


def turn(x, axis, by):
    return lax.ppermute(x, axis, [(i, (i + by) % SIDE) for i in range(SIDE)])


def neighbours(x, axis, count):
    pairs = [[(i, (i + 1) % count) for i in range(first, count, 2)] for first in range(2)]
    return tuple(lax.ppermute(x, axis, p + [(b, a) for a, b in p]) for p in pairs)


def on_device(update_basis, update_coeff, owner, sep_rhs, coupling, frontal_inverse):
    f_local = update_basis.shape[0]
    sep_size = update_basis.shape[3]
    rhs_count = update_coeff.shape[3]
    columns, rows = lax.axis_size(SX), lax.axis_size("sy")
    odd = [lax.rem(lax.axis_index(axis).astype(jnp.int32), 2) for axis in (SX, "sy")]
    freq_ids = [lax.axis_index("freq").astype(jnp.int32) * f_local + f + 1 for f in range(f_local)]
    place = [lax.axis_index(axis).astype(jnp.int32) for axis in SX]
    rows_of = [1 - odd[0], odd[0], 3 - odd[1], 2 + odd[1]]
    inside = []
    for axis, count in ((SX, columns), ("sy", rows)):
        at = lax.axis_index(axis)
        inside += [jnp.int32(1), ((at > 0) & (at < count - 1)).astype(jnp.int32)]
    table = jnp.stack(place + rows_of + inside + [i * i for i in freq_ids])
    data = (owner[:, 0], table, update_basis, update_coeff)
    half, full = jnp.bfloat16, jnp.float32

    axes = (SX, SX[::-1])
    plan = tuple((2 * f + n, 0, f, 2, pair) for f in range(2) for n, pair in enumerate((LOW, HIGH)))
    far = owner_products(plan, ((2, half),) * 4, *data, fetched=True)
    got = [(turn(far[2 * f], axes[f][0], 1), turn(far[2 * f + 1], axes[f][0], -1)) for f in range(2)]

    sides = ((1, LOW, HIGH), (3, HIGH, LOW))
    plan = tuple(
        (4 * late + 2 * f + n, 2 * late, f, ahead, pairs[late])
        for f in range(2)
        for n, (ahead, *pairs) in enumerate(sides)
        for late in range(2)
    )
    near = owner_products(plan, ((2, full),) * 4 + ((4, half),) * 4, *data)

    sums, joined = [], []
    for f in range(2):
        following = join(near[2 * f], got[f][0], near[4 + 2 * f])
        preceding = join(near[2 * f + 1], got[f][1], near[5 + 2 * f])
        joined += [following, preceding]
        sums.append((turn(following, axes[f][0], 1), turn(preceding, axes[f][0], -1)))
    plan = tuple((f, 2 * n, f, 0, pair) for f in range(2) for n, pair in enumerate((LOW, HIGH)))
    own = owner_products(plan, ((4, full),) * 2, *data, after=tuple(joined))
    rhs, matrix = staged(sep_rhs[:, 0, 0], frontal_inverse[:, 0, 0])

    coupling_rows = coupling[:, 0, 0]
    order = (1, 0)
    right_side, mine, sent = {}, {}, {}
    for f in order:
        here, following, preceding, opposite = row_totals(own[f], *sums[f])
        axis = axes[f][1]
        opposite = turn(opposite, axis, 2)
        beside = [
            turn(sums_of.astype(jnp.float16), axis, by).astype(full)
            for sums_of, by in ((following, 1), (preceding, -1))
        ]
        parts = (opposite, *beside)
        right_side[f], mine[f], sent[f] = first_solve(f, rhs, (here, *parts), matrix)
    for _ in range(SWEEPS - 1):
        for f in order:
            around = neighbours(sent[f], SX, columns) + neighbours(sent[f], "sy", rows)
            mine[f], sent[f] = sweep(f, table, right_side[f], mine[f], around, coupling_rows, matrix)
    group = ("sy", "freq")
    done = ()
    for f in order:
        around = neighbours(sent[f], SX, columns) + neighbours(sent[f], "sy", rows)
        done = last_sweep(
            f, table, right_side[f], mine[f], around, coupling_rows, matrix, done, lax.axis_size(group)
        )
    solution, squares = done
    squares = jnp.sum(lax.all_to_all(squares, group, 0, 0, tiled=True), axis=0)
    squares = jnp.broadcast_to(squares, (columns, *squares.shape))
    squares = jnp.sum(lax.all_to_all(squares, SX, 0, 0, tiled=True), axis=0)
    entries = float(f_local * lax.axis_size("freq") * columns * rows * sep_size * rhs_count)
    residual_total = jnp.sqrt(squares[0, 0] / entries + 1e-06)
    return (solution[:, None, None], residual_total)


def solution(mesh):
    finer = Mesh(
        mesh.devices.reshape(SIDE, SIDE, mesh.shape["sy"], mesh.shape["freq"]),
        ("sx_0", "sx_1", "sy", "freq"),
    )

    return jax.shard_map(
        on_device,
        mesh=finer,
        in_specs=(
            P("freq", SX_SY, None, None),
            P("freq", SX_SY, None, None),
            P(SX_SY, None),
            P("freq", SX, "sy", None, None),
            P("freq", SX, "sy", None, None),
            P("freq", SX, "sy", None, None),
        ),
        out_specs=(P("freq", SX, "sy", None, None), P()),
        check_vma=False,
    )
```

```python
import jax
import jax.numpy as jnp
from jax import lax
from jax.experimental import pallas as pl
from jax.experimental.pallas import tpu as pltpu
from jax.sharding import Mesh
from jax.sharding import PartitionSpec as P


SWEEPS = 2
SIDE = 4
CAP = 4
TILE = 256
SPARE = 16
SX = ("sx_0", "sx_1")
SX_SY = ("sx_0", "sx_1", "sy")
LOW, HIGH = (0, 1), (3, 2)


def cost(flops, bytes_accessed):
    return pl.CostEstimate(flops=flops, bytes_accessed=bytes_accessed, transcendentals=0)


def room(mebibytes):
    return pltpu.CompilerParams(vmem_limit_bytes=mebibytes << 20)


def fill_slots(owner_ref, slots, used):
    children = owner_ref.shape[0]
    for o in range(SIDE * SIDE):
        used[o] = 0
    for s in range(SIDE * SIDE * CAP):
        slots[s] = children

    def put(c, carry):
        o = owner_ref[c]
        k = used[o]
        slots[o * CAP + k] = c
        used[o] = k + 1
        return carry

    lax.fori_loop(0, children, put, 0)


def owner_at(table_ref, f, ahead, beside):
    offsets = (ahead, beside) if f == 0 else (beside, ahead)
    row = lax.rem(table_ref[0] + offsets[0], SIDE)
    column = lax.rem(table_ref[1] + offsets[1], SIDE)
    return row * SIDE + column


def multiply(weights, stacked, out, at):
    rhs_count = out.shape[1]
    turned = weights[...].T
    for s in range(0, stacked.shape[1], TILE):
        product = jnp.dot(turned, stacked[:, s : s + TILE], preferred_element_type=jnp.float32)
        for b in range(2):
            piece = product[b * rhs_count : (b + 1) * rhs_count]
            out[at + b, :, s : s + TILE] = piece.astype(out.dtype)


def put_weights(weights, coeff_ref, f, c, filled, b, k):
    rank, rhs_count = coeff_ref.shape[2:]
    at = (b * CAP + k) * rank
    coeff = coeff_ref[f, c]
    weights[at : at + rank, b * rhs_count : (b + 1) * rhs_count] = jnp.where(
        filled, coeff, jnp.zeros_like(coeff)
    )


def owner_products(plan, shapes, owners, place, basis, coeff, after=(), fetched=False):
    _, children, rank, sep_size = basis.shape
    rhs_count = coeff.shape[3]
    count = len(plan) if fetched else 1
    depth = 2 * CAP * rank

    def body(owner_ref, table_ref, basis_ref, coeff_ref, *rest):
        outs = rest[len(after) : len(after) + len(shapes)]
        slots, used, stacked, weights = rest[len(after) + len(shapes) :][:4]
        arrived = rest[-1]
        fill_slots(owner_ref, slots, used)

        def child(f, ahead, beside, k):
            c = slots[owner_at(table_ref, f, ahead, beside) * CAP + k]
            filled = c < children
            return jnp.where(filled, c, 0), filled

        def copies(n):
            _, _, f, ahead, pair = plan[n]
            return [
                pltpu.make_async_copy(
                    basis_ref.at[f, child(f, ahead, beside, k)[0]],
                    stacked.at[n, pl.ds((b * CAP + k) * rank, rank)],
                    arrived.at[n],
                )
                for b, beside in enumerate(pair)
                for k in range(CAP)
            ]

        if fetched:
            flights = [copies(n) for n in range(len(plan))]
            for flight in flights:
                for copy in flight:
                    copy.start()
        weights[...] = jnp.zeros_like(weights)
        for n, (out, at, f, ahead, pair) in enumerate(plan):
            for b, beside in enumerate(pair):
                for k in range(CAP):
                    c, filled = child(f, ahead, beside, k)
                    put_weights(weights, coeff_ref, f, c, filled, b, k)
                    if not fetched:
                        stacked[0, pl.ds((b * CAP + k) * rank, rank)] = basis_ref[f, c]
            if fetched:
                for copy in flights[n]:
                    copy.wait()
            multiply(weights, stacked.at[n if fetched else 0], outs[out], at)

    space = pltpu.MemorySpace.HBM if fetched else pltpu.MemorySpace.VMEM
    return pl.pallas_call(
        body,
        in_specs=[pl.BlockSpec(memory_space=pltpu.MemorySpace.SMEM)] * 2
        + [pl.BlockSpec(memory_space=space), pl.BlockSpec(memory_space=pltpu.MemorySpace.VMEM)]
        + [pl.BlockSpec(memory_space=pl.ANY) for _ in after],
        out_specs=[pl.BlockSpec(memory_space=pltpu.MemorySpace.VMEM) for _ in shapes],
        scratch_shapes=[
            pltpu.SMEM((SIDE * SIDE * CAP,), jnp.int32),
            pltpu.SMEM((SIDE * SIDE,), jnp.int32),
            pltpu.VMEM((count, depth, sep_size), jnp.bfloat16),
            pltpu.VMEM((depth, 2 * rhs_count), jnp.bfloat16),
            pltpu.SemaphoreType.DMA((count,)),
        ],
        out_shape=[jax.ShapeDtypeStruct((n, rhs_count, sep_size), dtype) for n, dtype in shapes],
        compiler_params=room(53 if fetched else 16),
        cost_estimate=cost(
            2 * len(plan) * 4 * CAP * rank * sep_size * rhs_count * 2,
            len(plan) * 2 * (CAP * rank * sep_size * 2 + rhs_count * sep_size * 4),
        ),
    )(owners, place, basis, coeff, *after)


def in_vmem(count):
    return [pl.BlockSpec(memory_space=pltpu.MemorySpace.VMEM)] * count


def join(mine, got, whole):
    def body(mine_ref, got_ref, whole_ref, out_ref):
        n = mine_ref.shape[0]
        out_ref[:n] = (mine_ref[...] + got_ref[...].astype(jnp.float32)).astype(out_ref.dtype)

    return pl.pallas_call(
        body,
        in_specs=in_vmem(3),
        out_specs=in_vmem(1)[0],
        out_shape=jax.ShapeDtypeStruct(whole.shape, whole.dtype),
        input_output_aliases={2: 0},
        compiler_params=room(4),
        cost_estimate=cost(mine.size * 2, mine.size * 8),
    )(mine, got, whole)


def row_totals(own, low, high):
    _, rhs_count, sep_size = own.shape

    def body(own_ref, low_ref, high_ref, here, following, preceding, opposite):
        def total(at):
            crossed = (at + 2) % SIDE
            return own_ref[at] + low_ref[at].astype(jnp.float32) + high_ref[crossed].astype(jnp.float32)

        here[...] = total(0)
        for at, out in ((1, following), (2, preceding)):
            sums = total(at)
            largest = jnp.max(jnp.abs(sums), axis=0, keepdims=True)
            largest = jnp.broadcast_to(jnp.max(largest), (SPARE, sep_size))
            power = jnp.clip(14.0 - jnp.ceil(jnp.log2(largest)), -60.0, 100.0)
            out[:rhs_count] = sums * jnp.exp2(power[:1])
            out[rhs_count:] = power
        opposite[...] = total(3).astype(jnp.bfloat16)

    plain = (rhs_count, sep_size)
    wide = (rhs_count + SPARE, sep_size)
    return pl.pallas_call(
        body,
        in_specs=in_vmem(3),
        out_specs=in_vmem(SIDE),
        out_shape=[jax.ShapeDtypeStruct(shape, jnp.float32) for shape in (plain, wide, wide)]
        + [jax.ShapeDtypeStruct(plain, jnp.bfloat16)],
        compiler_params=room(4),
        cost_estimate=cost(own.size * 2, own.size * 12),
    )(own, low, high)


def across(field, matrix_tile):
    return lax.dot_general(
        field, matrix_tile, (((1,), (1,)), ((), ())), preferred_element_type=jnp.float32
    )


def staged(sep_rhs, matrix):
    f_local, sep_size, rhs_count = sep_rhs.shape

    def body(rhs_ref, matrix_ref, out_ref, held_ref):
        for f in range(f_local):
            for s in range(0, sep_size, TILE):
                out_ref[f, :, s : s + TILE] = rhs_ref[f, s : s + TILE, :].astype(jnp.float32).T
                held_ref[f, s : s + TILE] = matrix_ref[f, s : s + TILE]

    return pl.pallas_call(
        body,
        in_specs=in_vmem(2),
        out_specs=in_vmem(2),
        out_shape=[
            jax.ShapeDtypeStruct((f_local, rhs_count, sep_size), jnp.float32),
            jax.ShapeDtypeStruct(matrix.shape, matrix.dtype),
        ],
        compiler_params=room(4),
        cost_estimate=cost(sep_rhs.size, sep_rhs.size * 6 + matrix.size * 4),
    )(sep_rhs, matrix)


def solve_cost(rhs_count, sep_size):
    return cost(2 * sep_size * sep_size * rhs_count, sep_size * (2 * sep_size + 24 * rhs_count))


def first_solve(f, rhs, parts, matrix):
    _, rhs_count, sep_size = rhs.shape

    def body(rhs_ref, *rest):
        parts_refs, (matrix_ref, right_ref, out_ref, sent_ref) = rest[:-4], rest[-4:]
        here, opposite, *beside = parts_refs
        right = rhs_ref[f] - here[...] - opposite[...].astype(jnp.float32)
        for part in beside:
            right = right - part[:rhs_count] * jnp.exp2(-part[rhs_count : rhs_count + 1])
        right_ref[...] = right
        field = right.astype(jnp.bfloat16)
        for s in range(0, sep_size, TILE):
            out = across(field, matrix_ref[f, s : s + TILE])
            out_ref[:, s : s + TILE] = out
            sent_ref[:, s : s + TILE] = out.astype(jnp.bfloat16)

    types = (jnp.float32, jnp.float32, jnp.bfloat16)
    return pl.pallas_call(
        body,
        in_specs=in_vmem(2 + len(parts)),
        out_specs=in_vmem(3),
        out_shape=[jax.ShapeDtypeStruct((rhs_count, sep_size), t) for t in types],
        compiler_params=room(6),
        cost_estimate=solve_cost(rhs_count, sep_size),
    )(rhs, *parts, matrix)


def residual_of(f, table_ref, right_ref, mine_ref, around_refs, coupling_ref):
    residual = right_ref[...] - mine_ref[...]
    for n, around in enumerate(around_refs):
        coupled = coupling_ref[f, pl.ds(table_ref[2 + n], 1), :]
        coupled = jnp.where(table_ref[6 + n] > 0, coupled, jnp.zeros_like(coupled))
        residual = residual + coupled * around[...].astype(jnp.float32)
    return residual


def sweep(f, table, right_side, mine, around, coupling, matrix):
    rhs_count, sep_size = mine.shape

    def body(table_ref, right_ref, mine_ref, *rest):
        around_refs, (coupling_ref, matrix_ref, out_ref, sent_ref) = rest[:4], rest[4:]
        residual = residual_of(f, table_ref, right_ref, mine_ref, around_refs, coupling_ref)
        field = residual.astype(jnp.bfloat16)
        for s in range(0, sep_size, TILE):
            out = mine_ref[:, s : s + TILE] + across(field, matrix_ref[f, s : s + TILE])
            out_ref[:, s : s + TILE] = out
            sent_ref[:, s : s + TILE] = out.astype(jnp.bfloat16)

    return pl.pallas_call(
        body,
        in_specs=[pl.BlockSpec(memory_space=pltpu.MemorySpace.SMEM)] + in_vmem(8),
        out_specs=in_vmem(2),
        out_shape=[jax.ShapeDtypeStruct(mine.shape, t) for t in (jnp.float32, jnp.bfloat16)],
        compiler_params=room(6),
        cost_estimate=solve_cost(rhs_count, sep_size),
    )(table, right_side, mine, *around, coupling, matrix)


def last_sweep(f, table, right_side, mine, around, coupling, matrix, before, copies):
    rhs_count, sep_size = mine.shape
    f_local = matrix.shape[0]

    def body(table_ref, right_ref, mine_ref, *rest):
        around_refs, (coupling_ref, matrix_ref), rest = rest[:4], rest[4:6], rest[6:]
        out_ref, sum_ref = rest[len(before) :]
        residual = residual_of(f, table_ref, right_ref, mine_ref, around_refs, coupling_ref)
        field = residual.astype(jnp.bfloat16)
        square = jnp.sum(residual * residual, axis=0, keepdims=True)
        total = jnp.sum(square * table_ref[10 + f].astype(jnp.float32))
        total = jnp.broadcast_to(total, sum_ref.shape)
        sum_ref[...] = total + rest[1][...] if before else total
        for s in range(0, sep_size, TILE):
            step = across(matrix_ref[f, s : s + TILE], field)
            out_ref[0, s : s + TILE, :] = mine_ref[:, s : s + TILE].T + step

    return pl.pallas_call(
        body,
        grid=(1,),
        in_specs=[pl.BlockSpec(memory_space=pltpu.MemorySpace.SMEM)]
        + in_vmem(8)
        + ([pl.BlockSpec(memory_space=pl.ANY)] + in_vmem(1) if before else []),
        out_specs=[pl.BlockSpec((1, sep_size, rhs_count), lambda i: (f, 0, 0)), in_vmem(1)[0]],
        out_shape=[
            jax.ShapeDtypeStruct((f_local, sep_size, rhs_count), jnp.float32),
            jax.ShapeDtypeStruct((copies, 8, 128), jnp.float32),
        ],
        input_output_aliases={9: 0} if before else {},
        compiler_params=room(6),
        cost_estimate=solve_cost(rhs_count, sep_size),
    )(table, right_side, mine, *around, coupling, matrix, *before)


def turn(x, axis, by):
    return lax.ppermute(x, axis, [(i, (i + by) % SIDE) for i in range(SIDE)])


def neighbours(x, axis, count):
    pairs = [[(i, (i + 1) % count) for i in range(first, count, 2)] for first in range(2)]
    return tuple(lax.ppermute(x, axis, p + [(b, a) for a, b in p]) for p in pairs)


def on_device(update_basis, update_coeff, owner, sep_rhs, coupling, frontal_inverse):
    f_local = update_basis.shape[0]
    sep_size = update_basis.shape[3]
    rhs_count = update_coeff.shape[3]
    columns, rows = lax.axis_size(SX), lax.axis_size("sy")
    odd = [lax.rem(lax.axis_index(axis).astype(jnp.int32), 2) for axis in (SX, "sy")]
    freq_ids = [lax.axis_index("freq").astype(jnp.int32) * f_local + f + 1 for f in range(f_local)]
    place = [lax.axis_index(axis).astype(jnp.int32) for axis in SX]
    rows_of = [1 - odd[0], odd[0], 3 - odd[1], 2 + odd[1]]
    inside = []
    for axis, count in ((SX, columns), ("sy", rows)):
        at = lax.axis_index(axis)
        inside += [jnp.int32(1), ((at > 0) & (at < count - 1)).astype(jnp.int32)]
    table = jnp.stack(place + rows_of + inside + [i * i for i in freq_ids])
    data = (owner[:, 0], table, update_basis, update_coeff)
    half, full = jnp.bfloat16, jnp.float32

    axes = (SX, SX[::-1])
    plan = tuple((2 * f + n, 0, f, 2, pair) for f in range(2) for n, pair in enumerate((LOW, HIGH)))
    far = owner_products(plan, ((2, half),) * 4, *data, fetched=True)
    got = []
    for f in range(2):
        got.append((turn(far[2 * f], axes[f][0], 1), turn(far[2 * f + 1], axes[f][0], -1)))

    sides = ((1, LOW, HIGH), (3, HIGH, LOW))
    plan = tuple(
        (4 * late + 2 * f + n, 2 * late, f, ahead, pairs[late])
        for f in range(2)
        for n, (ahead, *pairs) in enumerate(sides)
        for late in range(2)
    )
    near = owner_products(plan, ((2, full),) * 4 + ((4, half),) * 4, *data)

    sums, joined = [], []
    for f in range(2):
        following = join(near[2 * f], got[f][0], near[4 + 2 * f])
        preceding = join(near[2 * f + 1], got[f][1], near[5 + 2 * f])
        joined += [following, preceding]
        sums.append((turn(following, axes[f][0], 1), turn(preceding, axes[f][0], -1)))
    plan = tuple((f, 2 * n, f, 0, pair) for f in range(2) for n, pair in enumerate((LOW, HIGH)))
    own = owner_products(plan, ((4, full),) * 2, *data, after=tuple(joined))
    rhs, matrix = staged(sep_rhs[:, 0, 0], frontal_inverse[:, 0, 0])

    coupling_rows = coupling[:, 0, 0]
    order = (0, 1)
    right_side, mine, sent = {}, {}, {}
    for f in order:
        here, following, preceding, opposite = row_totals(own[f], *sums[f])
        axis = axes[f][1]
        opposite = turn(opposite, axis, 2)
        beside = [
            turn(sums_of.astype(jnp.float16), axis, by).astype(full)
            for sums_of, by in ((following, 1), (preceding, -1))
        ]
        parts = (opposite, *beside)
        right_side[f], mine[f], sent[f] = first_solve(f, rhs, (here, *parts), matrix)
    for _ in range(SWEEPS - 1):
        for f in order:
            around = neighbours(sent[f], SX, columns) + neighbours(sent[f], "sy", rows)
            mine[f], sent[f] = sweep(f, table, right_side[f], mine[f], around, coupling_rows, matrix)
    group = ("sy", "freq")
    done = ()
    for f in order:
        around = neighbours(sent[f], SX, columns) + neighbours(sent[f], "sy", rows)
        done = last_sweep(
            f, table, right_side[f], mine[f], around, coupling_rows, matrix, done, lax.axis_size(group)
        )
    solution, squares = done
    squares = jnp.sum(lax.all_to_all(squares, group, 0, 0, tiled=True), axis=0)
    squares = jnp.broadcast_to(squares, (columns, *squares.shape))
    squares = jnp.sum(lax.all_to_all(squares, SX, 0, 0, tiled=True), axis=0)
    entries = float(f_local * lax.axis_size("freq") * columns * rows * sep_size * rhs_count)
    residual_total = jnp.sqrt(squares[0, 0] / entries + 1e-06)
    return (solution[:, None, None], residual_total)


def solution(mesh):
    finer = Mesh(
        mesh.devices.reshape(SIDE, SIDE, mesh.shape["sy"], mesh.shape["freq"]),
        ("sx_0", "sx_1", "sy", "freq"),
    )

    return jax.shard_map(
        on_device,
        mesh=finer,
        in_specs=(
            P("freq", SX_SY, None, None),
            P("freq", SX_SY, None, None),
            P(SX_SY, None),
            P("freq", SX, "sy", None, None),
            P("freq", SX, "sy", None, None),
            P("freq", SX, "sy", None, None),
        ),
        out_specs=(P("freq", SX, "sy", None, None), P()),
        check_vma=False,
    )
```

```python
import functools

import jax
import jax.numpy as jnp
from jax import lax
from jax.experimental import pallas as pl
from jax.experimental.pallas import tpu as pltpu
from jax.sharding import Mesh
from jax.sharding import PartitionSpec as P


SWEEPS = 2
SIDE = 4
CAP = 4
TILE = 256
SPARE = 16
SX = ("sx_0", "sx_1")
SX_SY = ("sx_0", "sx_1", "sy")
LOW, HIGH = (0, 1), (3, 2)


def cost(flops, bytes_accessed):
    return pl.CostEstimate(flops=flops, bytes_accessed=bytes_accessed, transcendentals=0)


def room(mebibytes):
    return pltpu.CompilerParams(vmem_limit_bytes=mebibytes << 20)


def fill_slots(owner_ref, slots, used):
    children = owner_ref.shape[0]
    for o in range(SIDE * SIDE):
        used[o] = 0
    for s in range(SIDE * SIDE * CAP):
        slots[s] = children

    def put(c, carry):
        o = owner_ref[c]
        k = used[o]
        slots[o * CAP + k] = c
        used[o] = k + 1
        return carry

    lax.fori_loop(0, children, put, 0)


def owner_at(table_ref, f, ahead, beside):
    offsets = (ahead, beside) if f == 0 else (beside, ahead)
    row = lax.rem(table_ref[0] + offsets[0], SIDE)
    column = lax.rem(table_ref[1] + offsets[1], SIDE)
    return row * SIDE + column


def multiply(weights, stacked, out, at):
    rhs_count = out.shape[1]
    turned = weights[...].T
    for s in range(0, stacked.shape[1], TILE):
        product = jnp.dot(turned, stacked[:, s : s + TILE], preferred_element_type=jnp.float32)
        for b in range(2):
            piece = product[b * rhs_count : (b + 1) * rhs_count]
            out[at + b, :, s : s + TILE] = piece.astype(out.dtype)


def put_weights(weights, coeff_ref, f, c, filled, b, k):
    rank, rhs_count = coeff_ref.shape[2:]
    at = (b * CAP + k) * rank
    coeff = coeff_ref[f, c]
    weights[at : at + rank, b * rhs_count : (b + 1) * rhs_count] = jnp.where(
        filled, coeff, jnp.zeros_like(coeff)
    )


def owner_products(plan, shapes, owners, place, basis, coeff, after=(), fetched=False):
    _, children, rank, sep_size = basis.shape
    rhs_count = coeff.shape[3]
    count = len(plan) if fetched else 1
    depth = 2 * CAP * rank

    def body(owner_ref, table_ref, basis_ref, coeff_ref, *rest):
        outs = rest[len(after) : len(after) + len(shapes)]
        slots, used, stacked, weights = rest[len(after) + len(shapes) :][:4]
        arrived = rest[-1]
        fill_slots(owner_ref, slots, used)

        def child(f, ahead, beside, k):
            c = slots[owner_at(table_ref, f, ahead, beside) * CAP + k]
            filled = c < children
            return jnp.where(filled, c, 0), filled

        def copies(n):
            _, _, f, ahead, pair = plan[n]
            return [
                pltpu.make_async_copy(
                    basis_ref.at[f, child(f, ahead, beside, k)[0]],
                    stacked.at[n, pl.ds((b * CAP + k) * rank, rank)],
                    arrived.at[n],
                )
                for b, beside in enumerate(pair)
                for k in range(CAP)
            ]

        if fetched:
            flights = [copies(n) for n in range(len(plan))]
            for flight in flights:
                for copy in flight:
                    copy.start()
        weights[...] = jnp.zeros_like(weights)
        for n, (out, at, f, ahead, pair) in enumerate(plan):
            for b, beside in enumerate(pair):
                for k in range(CAP):
                    c, filled = child(f, ahead, beside, k)
                    put_weights(weights, coeff_ref, f, c, filled, b, k)
                    if not fetched:
                        stacked[0, pl.ds((b * CAP + k) * rank, rank)] = basis_ref[f, c]
            if fetched:
                for copy in flights[n]:
                    copy.wait()
            multiply(weights, stacked.at[n if fetched else 0], outs[out], at)

    space = pltpu.MemorySpace.HBM if fetched else pltpu.MemorySpace.VMEM
    return pl.pallas_call(
        body,
        in_specs=[pl.BlockSpec(memory_space=pltpu.MemorySpace.SMEM)] * 2
        + [pl.BlockSpec(memory_space=space), pl.BlockSpec(memory_space=pltpu.MemorySpace.VMEM)]
        + [pl.BlockSpec(memory_space=pl.ANY) for _ in after],
        out_specs=[pl.BlockSpec(memory_space=pltpu.MemorySpace.VMEM) for _ in shapes],
        scratch_shapes=[
            pltpu.SMEM((SIDE * SIDE * CAP,), jnp.int32),
            pltpu.SMEM((SIDE * SIDE,), jnp.int32),
            pltpu.VMEM((count, depth, sep_size), jnp.bfloat16),
            pltpu.VMEM((depth, 2 * rhs_count), jnp.bfloat16),
            pltpu.SemaphoreType.DMA((count,)),
        ],
        out_shape=[jax.ShapeDtypeStruct((n, rhs_count, sep_size), dtype) for n, dtype in shapes],
        compiler_params=room(53 if fetched else 16),
        cost_estimate=cost(
            2 * len(plan) * 4 * CAP * rank * sep_size * rhs_count * 2,
            len(plan) * 2 * (CAP * rank * sep_size * 2 + rhs_count * sep_size * 4),
        ),
    )(owners, place, basis, coeff, *after)


def in_vmem(count):
    return [pl.BlockSpec(memory_space=pltpu.MemorySpace.VMEM)] * count


def join(mine, got, whole):
    def body(mine_ref, got_ref, whole_ref, out_ref):
        n = mine_ref.shape[0]
        out_ref[:n] = (mine_ref[...] + got_ref[...].astype(jnp.float32)).astype(out_ref.dtype)

    return pl.pallas_call(
        body,
        in_specs=in_vmem(3),
        out_specs=in_vmem(1)[0],
        out_shape=jax.ShapeDtypeStruct(whole.shape, whole.dtype),
        input_output_aliases={2: 0},
        compiler_params=room(4),
        cost_estimate=cost(mine.size * 2, mine.size * 8),
    )(mine, got, whole)


def row_totals(own, low, high):
    _, rhs_count, sep_size = own.shape

    def body(own_ref, low_ref, high_ref, here, following, preceding, opposite):
        def total(at):
            crossed = (at + 2) % SIDE
            return own_ref[at] + low_ref[at].astype(jnp.float32) + high_ref[crossed].astype(jnp.float32)

        here[...] = total(0)
        for at, out in ((1, following), (2, preceding)):
            sums = total(at)
            largest = jnp.max(jnp.abs(sums), axis=0, keepdims=True)
            largest = jnp.broadcast_to(jnp.max(largest), (SPARE, sep_size))
            power = jnp.clip(14.0 - jnp.ceil(jnp.log2(largest)), -60.0, 100.0)
            out[:rhs_count] = sums * jnp.exp2(power[:1])
            out[rhs_count:] = power
        opposite[...] = total(3).astype(jnp.bfloat16)

    plain = (rhs_count, sep_size)
    wide = (rhs_count + SPARE, sep_size)
    return pl.pallas_call(
        body,
        in_specs=in_vmem(3),
        out_specs=in_vmem(SIDE),
        out_shape=[jax.ShapeDtypeStruct(shape, jnp.float32) for shape in (plain, wide, wide)]
        + [jax.ShapeDtypeStruct(plain, jnp.bfloat16)],
        compiler_params=room(4),
        cost_estimate=cost(own.size * 2, own.size * 12),
    )(own, low, high)


def across(field, matrix_tile):
    return lax.dot_general(
        field, matrix_tile, (((1,), (1,)), ((), ())), preferred_element_type=jnp.float32
    )


def staged(sep_rhs, matrix):
    f_local, sep_size, rhs_count = sep_rhs.shape

    def body(rhs_ref, matrix_ref, out_ref, held_ref):
        for f in range(f_local):
            for s in range(0, sep_size, TILE):
                out_ref[f, :, s : s + TILE] = rhs_ref[f, s : s + TILE, :].astype(jnp.float32).T
                held_ref[f, s : s + TILE] = matrix_ref[f, s : s + TILE]

    return pl.pallas_call(
        body,
        in_specs=in_vmem(2),
        out_specs=in_vmem(2),
        out_shape=[
            jax.ShapeDtypeStruct((f_local, rhs_count, sep_size), jnp.float32),
            jax.ShapeDtypeStruct(matrix.shape, matrix.dtype),
        ],
        compiler_params=room(4),
        cost_estimate=cost(sep_rhs.size, sep_rhs.size * 6 + matrix.size * 4),
    )(sep_rhs, matrix)


def first_solve(rhs, parts, matrix):
    f_local, rhs_count, sep_size = rhs.shape

    def body(rhs_ref, *rest):
        parts_refs, (matrix_ref, right_ref, out_ref, sent_ref) = rest[:-4], rest[-4:]
        for f in range(f_local):
            here, opposite, *beside = parts_refs[SIDE * f : SIDE * f + SIDE]
            right = rhs_ref[f] - here[...] - opposite[...].astype(jnp.float32)
            for part in beside:
                right = right - part[:rhs_count] * jnp.exp2(-part[rhs_count : rhs_count + 1])
            right_ref[f] = right
            field = right.astype(jnp.bfloat16)
            for s in range(0, sep_size, TILE):
                out = across(field, matrix_ref[f, s : s + TILE])
                out_ref[f, :, s : s + TILE] = out
                sent_ref[f, :, s : s + TILE] = out.astype(jnp.bfloat16)

    return pl.pallas_call(
        body,
        in_specs=in_vmem(2 + len(parts)),
        out_specs=in_vmem(3),
        out_shape=[jax.ShapeDtypeStruct(rhs.shape, t) for t in (jnp.float32, jnp.float32, jnp.bfloat16)],
        compiler_params=room(8),
        cost_estimate=cost(2 * matrix.size * rhs_count, matrix.size * 2 + rhs.size * 24),
    )(rhs, *parts, matrix)


def residual_of(f, table_ref, right_ref, mine_ref, around_refs, coupling_ref):
    residual = right_ref[f] - mine_ref[f]
    for n, around in enumerate(around_refs):
        coupled = coupling_ref[f, pl.ds(table_ref[2 + n], 1), :]
        coupled = jnp.where(table_ref[6 + n] > 0, coupled, jnp.zeros_like(coupled))
        residual = residual + coupled * around[f].astype(jnp.float32)
    return residual


def sweep(table, right_side, mine, around, coupling, matrix):
    f_local, rhs_count, sep_size = mine.shape

    def body(table_ref, right_ref, mine_ref, *rest):
        around_refs, (coupling_ref, matrix_ref, out_ref, sent_ref) = rest[:4], rest[4:]
        for f in range(f_local):
            residual = residual_of(f, table_ref, right_ref, mine_ref, around_refs, coupling_ref)
            field = residual.astype(jnp.bfloat16)
            for s in range(0, sep_size, TILE):
                out = mine_ref[f, :, s : s + TILE] + across(field, matrix_ref[f, s : s + TILE])
                out_ref[f, :, s : s + TILE] = out
                sent_ref[f, :, s : s + TILE] = out.astype(jnp.bfloat16)

    return pl.pallas_call(
        body,
        in_specs=[pl.BlockSpec(memory_space=pltpu.MemorySpace.SMEM)] + in_vmem(8),
        out_specs=in_vmem(2),
        out_shape=[jax.ShapeDtypeStruct(mine.shape, t) for t in (jnp.float32, jnp.bfloat16)],
        compiler_params=room(8),
        cost_estimate=cost(2 * matrix.size * rhs_count, matrix.size * 2 + mine.size * 24),
    )(table, right_side, mine, *around, coupling, matrix)


def last_sweep(table, right_side, mine, around, coupling, matrix, copies):
    f_local, rhs_count, sep_size = mine.shape

    def body(table_ref, right_ref, mine_ref, *rest):
        around_refs, (coupling_ref, matrix_ref, out_ref, sum_ref) = rest[:4], rest[4:]
        total = 0.0
        for f in range(f_local):
            residual = residual_of(f, table_ref, right_ref, mine_ref, around_refs, coupling_ref)
            field = residual.astype(jnp.bfloat16)
            square = jnp.sum(residual * residual, axis=0, keepdims=True)
            total = total + square * table_ref[10 + f].astype(jnp.float32)
            for s in range(0, sep_size, TILE):
                step = across(matrix_ref[f, s : s + TILE], field)
                out_ref[f, s : s + TILE, :] = mine_ref[f, :, s : s + TILE].T + step
        sum_ref[...] = jnp.broadcast_to(jnp.sum(total), sum_ref.shape)

    return pl.pallas_call(
        body,
        in_specs=[pl.BlockSpec(memory_space=pltpu.MemorySpace.SMEM)] + in_vmem(8),
        out_specs=in_vmem(2),
        out_shape=[
            jax.ShapeDtypeStruct((f_local, sep_size, rhs_count), jnp.float32),
            jax.ShapeDtypeStruct((copies, 8, 128), jnp.float32),
        ],
        compiler_params=room(8),
        cost_estimate=cost(2 * matrix.size * rhs_count, matrix.size * 2 + mine.size * 24),
    )(table, right_side, mine, *around, coupling, matrix)


def turn(x, axis, by):
    return lax.ppermute(x, axis, [(i, (i + by) % SIDE) for i in range(SIDE)])


def neighbours(x, axis, count):
    pairs = [[(i, (i + 1) % count) for i in range(first, count, 2)] for first in range(2)]
    return tuple(lax.ppermute(x, axis, p + [(b, a) for a, b in p]) for p in pairs)


def on_device(update_basis, update_coeff, owner, sep_rhs, coupling, frontal_inverse):
    f_local = update_basis.shape[0]
    sep_size = update_basis.shape[3]
    rhs_count = update_coeff.shape[3]
    columns, rows = lax.axis_size(SX), lax.axis_size("sy")
    odd = [lax.rem(lax.axis_index(axis).astype(jnp.int32), 2) for axis in (SX, "sy")]
    freq_ids = [lax.axis_index("freq").astype(jnp.int32) * f_local + f + 1 for f in range(f_local)]
    place = [lax.axis_index(axis).astype(jnp.int32) for axis in SX]
    rows_of = [1 - odd[0], odd[0], 3 - odd[1], 2 + odd[1]]
    inside = []
    for axis, count in ((SX, columns), ("sy", rows)):
        at = lax.axis_index(axis)
        inside += [jnp.int32(1), ((at > 0) & (at < count - 1)).astype(jnp.int32)]
    table = jnp.stack(place + rows_of + inside + [i * i for i in freq_ids])
    data = (owner[:, 0], table, update_basis, update_coeff)
    half, full = jnp.bfloat16, jnp.float32

    axes = (SX, SX[::-1])
    plan = tuple((2 * f + n, 0, f, 2, pair) for f in range(2) for n, pair in enumerate((LOW, HIGH)))
    far = owner_products(plan, ((2, half),) * 4, *data, fetched=True)
    got = [(turn(far[2 * f], axes[f][0], 1), turn(far[2 * f + 1], axes[f][0], -1)) for f in range(2)]

    sides = ((1, LOW, HIGH), (3, HIGH, LOW))
    plan = tuple(
        (4 * late + 2 * f + n, 2 * late, f, ahead, pairs[late])
        for f in range(2)
        for n, (ahead, *pairs) in enumerate(sides)
        for late in range(2)
    )
    near = owner_products(plan, ((2, full),) * 4 + ((4, half),) * 4, *data)

    sums, joined = [], []
    for f in range(2):
        following = join(near[2 * f], got[f][0], near[4 + 2 * f])
        preceding = join(near[2 * f + 1], got[f][1], near[5 + 2 * f])
        joined += [following, preceding]
        sums.append((turn(following, axes[f][0], 1), turn(preceding, axes[f][0], -1)))
    plan = tuple((f, 2 * n, f, 0, pair) for f in range(2) for n, pair in enumerate((LOW, HIGH)))
    own = owner_products(plan, ((4, full),) * 2, *data, after=tuple(joined))
    rhs, matrix = staged(sep_rhs[:, 0, 0], frontal_inverse[:, 0, 0])

    parts = []
    for f in range(2):
        here, following, preceding, opposite = row_totals(own[f], *sums[f])
        axis = axes[f][1]
        parts += [here, turn(opposite, axis, 2)] + [
            turn(sums_of.astype(jnp.float16), axis, by).astype(full)
            for sums_of, by in ((following, 1), (preceding, -1))
        ]

    coupling_rows = coupling[:, 0, 0]
    right_side, mine, sent = first_solve(rhs, parts, matrix)
    for _ in range(SWEEPS - 1):
        around = neighbours(sent, SX, columns) + neighbours(sent, "sy", rows)
        mine, sent = sweep(table, right_side, mine, around, coupling_rows, matrix)
    around = neighbours(sent, SX, columns) + neighbours(sent, "sy", rows)
    group = ("sy", "freq")
    solution, squares = last_sweep(
        table, right_side, mine, around, coupling_rows, matrix, lax.axis_size(group)
    )
    squares = jnp.sum(lax.all_to_all(squares, group, 0, 0, tiled=True), axis=0)
    squares = jnp.broadcast_to(squares, (columns, *squares.shape))
    squares = jnp.sum(lax.all_to_all(squares, SX, 0, 0, tiled=True), axis=0)
    entries = float(f_local * lax.axis_size("freq") * columns * rows * sep_size * rhs_count)
    residual_total = jnp.sqrt(squares[0, 0] / entries + 1e-06)
    return (solution[:, None, None], residual_total)


def solution(mesh):
    finer = Mesh(
        mesh.devices.reshape(SIDE, SIDE, mesh.shape["sy"], mesh.shape["freq"]),
        ("sx_0", "sx_1", "sy", "freq"),
    )
    return jax.shard_map(
        on_device,
        mesh=finer,
        in_specs=(
            P("freq", SX_SY, None, None),
            P("freq", SX_SY, None, None),
            P(SX_SY, None),
            P("freq", SX, "sy", None, None),
            P("freq", SX, "sy", None, None),
            P("freq", SX, "sy", None, None),
        ),
        out_specs=(P("freq", SX, "sy", None, None), P()),
        check_vma=False,
    )
```

```python
import functools

import jax
import jax.numpy as jnp
from jax import lax
from jax.experimental import pallas as pl
from jax.experimental.pallas import tpu as pltpu
from jax.sharding import Mesh
from jax.sharding import PartitionSpec as P


SWEEPS = 2
SIDE = 4
CAP = 4
TILE = 256
SPARE = 16
SX = ("sx_0", "sx_1")
SX_SY = ("sx_0", "sx_1", "sy")
LOW, HIGH = (0, 1), (3, 2)


def cost(flops, bytes_accessed):
    return pl.CostEstimate(flops=flops, bytes_accessed=bytes_accessed, transcendentals=0)


def room(mebibytes):
    return pltpu.CompilerParams(vmem_limit_bytes=mebibytes << 20)


def fill_slots(owner_ref, slots, used):
    children = owner_ref.shape[0]
    for o in range(SIDE * SIDE):
        used[o] = 0
    for s in range(SIDE * SIDE * CAP):
        slots[s] = children

    def put(c, carry):
        o = owner_ref[c]
        k = used[o]
        slots[o * CAP + k] = c
        used[o] = k + 1
        return carry

    lax.fori_loop(0, children, put, 0)


def owner_at(table_ref, f, ahead, beside):
    offsets = (ahead, beside) if f == 0 else (beside, ahead)
    row = lax.rem(table_ref[0] + offsets[0], SIDE)
    column = lax.rem(table_ref[1] + offsets[1], SIDE)
    return row * SIDE + column


def multiply(weights, stacked, out, at):
    rhs_count = out.shape[1]
    turned = weights[...].T
    for s in range(0, stacked.shape[1], TILE):
        product = jnp.dot(turned, stacked[:, s : s + TILE], preferred_element_type=jnp.float32)
        for b in range(2):
            piece = product[b * rhs_count : (b + 1) * rhs_count]
            out[at + b, :, s : s + TILE] = piece.astype(out.dtype)


def put_weights(weights, coeff_ref, f, c, filled, b, k):
    rank, rhs_count = coeff_ref.shape[2:]
    at = (b * CAP + k) * rank
    coeff = coeff_ref[f, c]
    weights[at : at + rank, b * rhs_count : (b + 1) * rhs_count] = jnp.where(
        filled, coeff, jnp.zeros_like(coeff)
    )


def owner_products(plan, shapes, owners, place, basis, coeff, after=(), fetched=False):
    _, children, rank, sep_size = basis.shape
    rhs_count = coeff.shape[3]
    count = len(plan) if fetched else 1
    depth = 2 * CAP * rank

    def body(owner_ref, table_ref, basis_ref, coeff_ref, *rest):
        outs = rest[len(after) : len(after) + len(shapes)]
        slots, used, stacked, weights = rest[len(after) + len(shapes) :][:4]
        arrived = rest[-1]
        fill_slots(owner_ref, slots, used)

        def child(f, ahead, beside, k):
            c = slots[owner_at(table_ref, f, ahead, beside) * CAP + k]
            filled = c < children
            return jnp.where(filled, c, 0), filled

        def copies(n):
            _, _, f, ahead, pair = plan[n]
            return [
                pltpu.make_async_copy(
                    basis_ref.at[f, child(f, ahead, beside, k)[0]],
                    stacked.at[n, pl.ds((b * CAP + k) * rank, rank)],
                    arrived.at[n],
                )
                for b, beside in enumerate(pair)
                for k in range(CAP)
            ]

        if fetched:
            flights = [copies(n) for n in range(len(plan))]
            for flight in flights:
                for copy in flight:
                    copy.start()
        weights[...] = jnp.zeros_like(weights)
        for n, (out, at, f, ahead, pair) in enumerate(plan):
            for b, beside in enumerate(pair):
                for k in range(CAP):
                    c, filled = child(f, ahead, beside, k)
                    put_weights(weights, coeff_ref, f, c, filled, b, k)
                    if not fetched:
                        stacked[0, pl.ds((b * CAP + k) * rank, rank)] = basis_ref[f, c]
            if fetched:
                for copy in flights[n]:
                    copy.wait()
            multiply(weights, stacked.at[n if fetched else 0], outs[out], at)

    space = pltpu.MemorySpace.HBM if fetched else pltpu.MemorySpace.VMEM
    return pl.pallas_call(
        body,
        in_specs=[pl.BlockSpec(memory_space=pltpu.MemorySpace.SMEM)] * 2
        + [pl.BlockSpec(memory_space=space), pl.BlockSpec(memory_space=pltpu.MemorySpace.VMEM)]
        + [pl.BlockSpec(memory_space=pl.ANY) for _ in after],
        out_specs=[pl.BlockSpec(memory_space=pltpu.MemorySpace.VMEM) for _ in shapes],
        scratch_shapes=[
            pltpu.SMEM((SIDE * SIDE * CAP,), jnp.int32),
            pltpu.SMEM((SIDE * SIDE,), jnp.int32),
            pltpu.VMEM((count, depth, sep_size), jnp.bfloat16),
            pltpu.VMEM((depth, 2 * rhs_count), jnp.bfloat16),
            pltpu.SemaphoreType.DMA((count,)),
        ],
        out_shape=[jax.ShapeDtypeStruct((n, rhs_count, sep_size), dtype) for n, dtype in shapes],
        compiler_params=room(53 if fetched else 16),
        cost_estimate=cost(
            2 * len(plan) * 4 * CAP * rank * sep_size * rhs_count * 2,
            len(plan) * 2 * (CAP * rank * sep_size * 2 + rhs_count * sep_size * 4),
        ),
    )(owners, place, basis, coeff, *after)


def in_vmem(count):
    return [pl.BlockSpec(memory_space=pltpu.MemorySpace.VMEM)] * count


def join(mine, got, whole):
    def body(mine_ref, got_ref, whole_ref, out_ref):
        n = mine_ref.shape[0]
        out_ref[:n] = (mine_ref[...] + got_ref[...].astype(jnp.float32)).astype(out_ref.dtype)

    return pl.pallas_call(
        body,
        in_specs=in_vmem(3),
        out_specs=in_vmem(1)[0],
        out_shape=jax.ShapeDtypeStruct(whole.shape, whole.dtype),
        input_output_aliases={2: 0},
        compiler_params=room(4),
        cost_estimate=cost(mine.size * 2, mine.size * 8),
    )(mine, got, whole)


def row_totals(own, low, high):
    _, rhs_count, sep_size = own.shape

    def body(own_ref, low_ref, high_ref, here, following, preceding, opposite):
        def total(at):
            crossed = (at + 2) % SIDE
            return own_ref[at] + low_ref[at].astype(jnp.float32) + high_ref[crossed].astype(jnp.float32)

        here[...] = total(0)
        for at, out in ((1, following), (2, preceding)):
            sums = total(at)
            largest = jnp.max(jnp.abs(sums), axis=0, keepdims=True)
            largest = jnp.broadcast_to(jnp.max(largest), (SPARE, sep_size))
            power = jnp.clip(14.0 - jnp.ceil(jnp.log2(largest)), -60.0, 100.0)
            out[:rhs_count] = sums * jnp.exp2(power[:1])
            out[rhs_count:] = power
        opposite[...] = total(3).astype(jnp.bfloat16)

    plain = (rhs_count, sep_size)
    wide = (rhs_count + SPARE, sep_size)
    return pl.pallas_call(
        body,
        in_specs=in_vmem(3),
        out_specs=in_vmem(SIDE),
        out_shape=[jax.ShapeDtypeStruct(shape, jnp.float32) for shape in (plain, wide, wide)]
        + [jax.ShapeDtypeStruct(plain, jnp.bfloat16)],
        compiler_params=room(4),
        cost_estimate=cost(own.size * 2, own.size * 12),
    )(own, low, high)


def across(field, matrix_tile):
    return lax.dot_general(
        field, matrix_tile, (((1,), (1,)), ((), ())), preferred_element_type=jnp.float32
    )


def staged(sep_rhs, matrix):
    f_local, sep_size, rhs_count = sep_rhs.shape

    def body(rhs_ref, matrix_ref, out_ref, held_ref):
        for f in range(f_local):
            for s in range(0, sep_size, TILE):
                out_ref[f, :, s : s + TILE] = rhs_ref[f, s : s + TILE, :].astype(jnp.float32).T
                held_ref[f, s : s + TILE] = matrix_ref[f, s : s + TILE]

    return pl.pallas_call(
        body,
        in_specs=in_vmem(2),
        out_specs=in_vmem(2),
        out_shape=[
            jax.ShapeDtypeStruct((f_local, rhs_count, sep_size), jnp.float32),
            jax.ShapeDtypeStruct(matrix.shape, matrix.dtype),
        ],
        compiler_params=room(4),
        cost_estimate=cost(sep_rhs.size, sep_rhs.size * 6 + matrix.size * 4),
    )(sep_rhs, matrix)


def first_solve(rhs, parts, matrix):
    f_local, rhs_count, sep_size = rhs.shape

    def body(rhs_ref, *rest):
        parts_refs, (matrix_ref, right_ref, out_ref, sent_ref) = rest[:-4], rest[-4:]
        for f in range(f_local):
            here, opposite, *beside = parts_refs[SIDE * f : SIDE * f + SIDE]
            right = rhs_ref[f] - here[...] - opposite[...].astype(jnp.float32)
            for part in beside:
                right = right - part[:rhs_count] * jnp.exp2(-part[rhs_count : rhs_count + 1])
            right_ref[f] = right
            field = right.astype(jnp.bfloat16)
            for s in range(0, sep_size, TILE):
                out = across(field, matrix_ref[f, s : s + TILE])
                out_ref[f, :, s : s + TILE] = out
                sent_ref[f, :, s : s + TILE] = out.astype(jnp.bfloat16)

    return pl.pallas_call(
        body,
        in_specs=in_vmem(2 + len(parts)),
        out_specs=in_vmem(3),
        out_shape=[jax.ShapeDtypeStruct(rhs.shape, t) for t in (jnp.float32, jnp.float32, jnp.bfloat16)],
        compiler_params=room(8),
        cost_estimate=cost(2 * matrix.size * rhs_count, matrix.size * 2 + rhs.size * 24),
    )(rhs, *parts, matrix)


def residual_of(f, table_ref, right_ref, mine_ref, around_refs, coupling_ref):
    residual = right_ref[f] - mine_ref[f]
    for n, around in enumerate(around_refs):
        coupled = coupling_ref[f, pl.ds(table_ref[2 + n], 1), :]
        coupled = jnp.where(table_ref[6 + n] > 0, coupled, jnp.zeros_like(coupled))
        residual = residual + coupled * around[f].astype(jnp.float32)
    return residual


def sweep(table, right_side, mine, around, coupling, matrix):
    f_local, rhs_count, sep_size = mine.shape

    def body(table_ref, right_ref, mine_ref, *rest):
        around_refs, (coupling_ref, matrix_ref, out_ref, sent_ref) = rest[:4], rest[4:]
        for f in range(f_local):
            residual = residual_of(f, table_ref, right_ref, mine_ref, around_refs, coupling_ref)
            field = residual.astype(jnp.bfloat16)
            for s in range(0, sep_size, TILE):
                out = mine_ref[f, :, s : s + TILE] + across(field, matrix_ref[f, s : s + TILE])
                out_ref[f, :, s : s + TILE] = out
                sent_ref[f, :, s : s + TILE] = out.astype(jnp.bfloat16)

    return pl.pallas_call(
        body,
        in_specs=[pl.BlockSpec(memory_space=pltpu.MemorySpace.SMEM)] + in_vmem(8),
        out_specs=in_vmem(2),
        out_shape=[jax.ShapeDtypeStruct(mine.shape, t) for t in (jnp.float32, jnp.bfloat16)],
        compiler_params=room(8),
        cost_estimate=cost(2 * matrix.size * rhs_count, matrix.size * 2 + mine.size * 24),
    )(table, right_side, mine, *around, coupling, matrix)


def last_sweep(table, right_side, mine, around, coupling, matrix, copies):
    f_local, rhs_count, sep_size = mine.shape

    def body(table_ref, right_ref, mine_ref, *rest):
        around_refs, (coupling_ref, matrix_ref, out_ref, sum_ref) = rest[:4], rest[4:]
        total = 0.0
        for f in range(f_local):
            residual = residual_of(f, table_ref, right_ref, mine_ref, around_refs, coupling_ref)
            field = residual.astype(jnp.bfloat16)
            square = jnp.sum(residual * residual, axis=0, keepdims=True)
            total = total + square * table_ref[10 + f].astype(jnp.float32)
            for s in range(0, sep_size, TILE):
                out = mine_ref[f, :, s : s + TILE] + across(field, matrix_ref[f, s : s + TILE])
                out_ref[f, s : s + TILE, :] = out.T
        sum_ref[...] = jnp.broadcast_to(jnp.sum(total), sum_ref.shape)

    return pl.pallas_call(
        body,
        in_specs=[pl.BlockSpec(memory_space=pltpu.MemorySpace.SMEM)] + in_vmem(8),
        out_specs=in_vmem(2),
        out_shape=[
            jax.ShapeDtypeStruct((f_local, sep_size, rhs_count), jnp.float32),
            jax.ShapeDtypeStruct((copies, 8, 128), jnp.float32),
        ],
        compiler_params=room(8),
        cost_estimate=cost(2 * matrix.size * rhs_count, matrix.size * 2 + mine.size * 24),
    )(table, right_side, mine, *around, coupling, matrix)


def turn(x, axis, by):
    return lax.ppermute(x, axis, [(i, (i + by) % SIDE) for i in range(SIDE)])


def neighbours(x, axis, count):
    pairs = [[(i, (i + 1) % count) for i in range(first, count, 2)] for first in range(2)]
    return tuple(lax.ppermute(x, axis, p + [(b, a) for a, b in p]) for p in pairs)


def on_device(update_basis, update_coeff, owner, sep_rhs, coupling, frontal_inverse):
    f_local = update_basis.shape[0]
    sep_size = update_basis.shape[3]
    rhs_count = update_coeff.shape[3]
    columns, rows = lax.axis_size(SX), lax.axis_size("sy")
    odd = [lax.rem(lax.axis_index(axis).astype(jnp.int32), 2) for axis in (SX, "sy")]
    freq_ids = [lax.axis_index("freq").astype(jnp.int32) * f_local + f + 1 for f in range(f_local)]
    place = [lax.axis_index(axis).astype(jnp.int32) for axis in SX]
    rows_of = [1 - odd[0], odd[0], 3 - odd[1], 2 + odd[1]]
    inside = []
    for axis, count in ((SX, columns), ("sy", rows)):
        at = lax.axis_index(axis)
        inside += [jnp.int32(1), ((at > 0) & (at < count - 1)).astype(jnp.int32)]
    table = jnp.stack(place + rows_of + inside + [i * i for i in freq_ids])
    data = (owner[:, 0], table, update_basis, update_coeff)
    half, full = jnp.bfloat16, jnp.float32

    axes = (SX, SX[::-1])
    plan = tuple((2 * f + n, 0, f, 2, pair) for f in range(2) for n, pair in enumerate((LOW, HIGH)))
    far = owner_products(plan, ((2, half),) * 4, *data, fetched=True)
    got = [(turn(far[2 * f], axes[f][0], 1), turn(far[2 * f + 1], axes[f][0], -1)) for f in range(2)]

    sides = ((1, LOW, HIGH), (3, HIGH, LOW))
    plan = tuple(
        (4 * late + 2 * f + n, 2 * late, f, ahead, pairs[late])
        for f in range(2)
        for n, (ahead, *pairs) in enumerate(sides)
        for late in range(2)
    )
    near = owner_products(plan, ((2, full),) * 4 + ((4, half),) * 4, *data)

    sums, joined = [], []
    for f in range(2):
        following = join(near[2 * f], got[f][0], near[4 + 2 * f])
        preceding = join(near[2 * f + 1], got[f][1], near[5 + 2 * f])
        joined += [following, preceding]
        sums.append((turn(following, axes[f][0], 1), turn(preceding, axes[f][0], -1)))
    plan = tuple((f, 2 * n, f, 0, pair) for f in range(2) for n, pair in enumerate((LOW, HIGH)))
    own = owner_products(plan, ((4, full),) * 2, *data, after=tuple(joined))
    rhs, matrix = staged(sep_rhs[:, 0, 0], frontal_inverse[:, 0, 0])

    parts = []
    for f in range(2):
        here, following, preceding, opposite = row_totals(own[f], *sums[f])
        axis = axes[f][1]
        parts += [here, turn(opposite, axis, 2)] + [
            turn(sums_of.astype(jnp.float16), axis, by).astype(full)
            for sums_of, by in ((following, 1), (preceding, -1))
        ]

    coupling_rows = coupling[:, 0, 0]
    right_side, mine, sent = first_solve(rhs, parts, matrix)
    for _ in range(SWEEPS - 1):
        around = neighbours(sent, SX, columns) + neighbours(sent, "sy", rows)
        mine, sent = sweep(table, right_side, mine, around, coupling_rows, matrix)
    around = neighbours(sent, SX, columns) + neighbours(sent, "sy", rows)
    group = ("sy", "freq")
    solution, squares = last_sweep(
        table, right_side, mine, around, coupling_rows, matrix, lax.axis_size(group)
    )
    squares = jnp.sum(lax.all_to_all(squares, group, 0, 0, tiled=True), axis=0)
    squares = jnp.broadcast_to(squares, (columns, *squares.shape))
    squares = jnp.sum(lax.all_to_all(squares, SX, 0, 0, tiled=True), axis=0)
    entries = float(f_local * lax.axis_size("freq") * columns * rows * sep_size * rhs_count)
    residual_total = jnp.sqrt(squares[0, 0] / entries + 1e-06)
    return (solution[:, None, None], residual_total)


def solution(mesh):
    finer = Mesh(
        mesh.devices.reshape(SIDE, SIDE, mesh.shape["sy"], mesh.shape["freq"]),
        ("sx_0", "sx_1", "sy", "freq"),
    )
    return jax.shard_map(
        on_device,
        mesh=finer,
        in_specs=(
            P("freq", SX_SY, None, None),
            P("freq", SX_SY, None, None),
            P(SX_SY, None),
            P("freq", SX, "sy", None, None),
            P("freq", SX, "sy", None, None),
            P("freq", SX, "sy", None, None),
        ),
        out_specs=(P("freq", SX, "sy", None, None), P()),
        check_vma=False,
    )
```
